256 devices in a mesh: sec: 8 (over y, x_lo), row: 32 (over z, x_hi, core).
Axes of the slice: x: 4 (x_hi: 2, x_lo: 2; x = x_hi * 2 + x_lo), y: 4, z: 8, core: 2. Of those that a mesh axis runs over, the one named last changes fastest.
Arguments:
- rhs: float32 [8192, 256], P(('sec', 'row')), may hold values from -6 to 6
- coupling: bfloat16 [8, 1024, 8192], P(None, 'row', 'sec'), may hold values from -0.0625 to 0.0625
- diag_inverse: bfloat16 [8, 1024, 1024], P('sec'), as said below
Outputs:
- solution: float32 [8192, 256], P(('sec', 'row'))
- forward: float32 [8192, 256], P(('sec', 'row'))
The draws below stay inside these ranges and needn't reach their ends.
Inputs may be any that keep to these rules, and one draw needn't show every extreme that they name: `diag_inverse`: each of the 8 blocks is lower triangular with diagonal entries from 0.5 to 1.5.
All inputs are finite; a program needn't handle non-finite values.
Results may differ from the reference program's by a relative error of at most 0.02.
Values may be sent and summed in bfloat16 or wider, within the bound.
No kernel may reach another device: no remote copies, remote signals or barrier semaphores. Data moves between devices by JAX's collectives and lax.ppermute only.
A program may use at most 64 MiB of HBM per device.

```python
import jax
import jax.numpy as jnp
from jax import lax

W = 1024
SECTIONS = 8
M = 8192
NRHS = 256
N_ROW = 32


def draw_diag_inverse(key, part):
    base = jax.random.fold_in(key, 11)
    first, second = jax.random.split(base)
    index = jnp.arange(W)
    lower = index[:, None] > index[None, :]
    below = jax.random.normal(first, (SECTIONS, W, W), jnp.float32) * (0.5 / W ** 0.5)
    diagonal = jnp.exp(jax.random.uniform(second, (SECTIONS, W), jnp.float32, jnp.log(0.5), jnp.log(1.5)))
    eye = (index[:, None] == index[None, :]).astype(jnp.float32)
    result = jnp.where(lower[None], below, 0.0) + eye[None] * diagonal[:, :, None]
    return result.astype(jnp.bfloat16)


def block_scale(key, extent, shards, smallest, high):
    loudness = 1.0
    for position, blocks in shards:
        heights = jax.random.uniform(jax.random.fold_in(jax.random.fold_in(key, 6), position), (blocks,), jnp.float32, smallest / len(shards), high / len(shards))
        loudness = loudness * jnp.repeat(jnp.exp(heights), extent[position] // blocks).reshape((-1,) + (1,) * (len(extent) - 1 - position))
    return loudness


def noise(key, extent, scale, bound, shards=(), dtype=jnp.bfloat16):
    level = block_scale(key, extent, shards, -0.22, 0.18) if shards else 1.0
    drawn = jax.random.normal(key, extent, jnp.float32) * scale * level
    return jnp.minimum(jnp.maximum(drawn, -bound), bound).astype(dtype)


def setup_inputs(seed: int = 0) -> dict:
    streams_of = jax.random.split(jax.random.key(seed), 4)
    return {
        "rhs": noise(streams_of[0], (M, NRHS), 1.0, 6.0, ((0, 256),), jnp.float32),
        "coupling": noise(streams_of[1], (SECTIONS, W, M), M ** -0.5, 0.0625, ((1, 32), (2, 8))),
        "diag_inverse": draw_diag_inverse(jax.random.fold_in(streams_of[3], 71), 0),
    }


def reference(rhs, coupling, diag_inverse):
    sections = SECTIONS
    width = W
    rows = W // N_ROW
    forward_parts = []
    low_forward = []
    for sec_now in range(sections):
        accum = jnp.zeros((width, NRHS), jnp.float32)
        for earlier in range(sec_now):
            block = coupling[sec_now, :, earlier * width:(earlier + 1) * width]
            accum = accum + jnp.dot(block, low_forward[earlier], preferred_element_type=jnp.float32)
        resid = (rhs[sec_now * width:(sec_now + 1) * width] - accum).astype(jnp.bfloat16)
        solved = jnp.dot(diag_inverse[sec_now], resid, preferred_element_type=jnp.float32)
        forward_parts.append(solved)
        low_forward.append(solved.astype(jnp.bfloat16))
    low_solution = [None] * sections
    solution_parts = [None] * sections
    for sec_now in range(sections - 1, -1, -1):
        partial_value = jnp.zeros((N_ROW, width, NRHS), jnp.float32)
        for later in range(sec_now + 1, sections):
            block = coupling[later, :, sec_now * width:(sec_now + 1) * width].astype(jnp.float32)
            block = block.reshape(N_ROW, rows, width)
            solved_later = low_solution[later].astype(jnp.float32).reshape(N_ROW, rows, NRHS)
            partial_value = partial_value + jnp.einsum('gjw,gjc->gwc', block, solved_later)
        rounded = lax.optimization_barrier(partial_value.astype(jnp.bfloat16))
        summed = jnp.sum(rounded.astype(jnp.float32), axis=0)
        lowered = (forward_parts[sec_now] - summed).astype(jnp.bfloat16)
        solved = lax.dot_general(diag_inverse[sec_now], lowered, (((0,), (0,)), ((), ())), preferred_element_type=jnp.float32)
        solution_parts[sec_now] = solved
        low_solution[sec_now] = solved.astype(jnp.bfloat16)
    return jnp.concatenate(solution_parts, axis=0), jnp.concatenate(forward_parts, axis=0)
```

```python
import jax
import jax.numpy as jnp
from jax import lax
from jax.sharding import PartitionSpec as P

BF = jnp.bfloat16
F32 = jnp.float32
SEC, ROW = 8, 32
NT = (((1,), (1,)), ((), ()))
NN = (((1,), (0,)), ((), ()))
BOTH = ("sec", "row")


def place(dev):
    sec, row = divmod(dev, ROW)
    return sec // 2, sec % 2, row // 4, (row // 2) % 2, row % 2


def device(y, xl, z, xh, core):
    return (y * 2 + xl) * ROW + z * 4 + xh * 2 + core


def ring(move):
    return [(d, device(*move(*place(d)))) for d in range(SEC * ROW)]


XL = ring(lambda y, xl, z, xh, k: (y, 1 - xl, z, xh, k))
XH = ring(lambda y, xl, z, xh, k: (y, xl, z, 1 - xh, k))
CORE = ring(lambda y, xl, z, xh, k: (y, xl, z, xh, 1 - k))
ZUP = ring(lambda y, xl, z, xh, k: (y, xl, (z + 1) % 8, xh, k))
ZDOWN = ring(lambda y, xl, z, xh, k: (y, xl, (z - 1) % 8, xh, k))
PLANES = [
    [device(y, xl, z, xh, k) for xl in range(2) for xh in range(2) for z in range(8)]
    for y in range(4)
    for k in range(2)
]
COLUMNS_Y = [[xl + 2 * y for y in range(4)] for xl in range(2)]


def send(x, pairs):
    return lax.ppermute(x, BOTH, pairs)


def dot(a, b, dims):
    return lax.dot_general(a, b, dims, preferred_element_type=F32)


def put(buffer, piece, dim, index):
    start = [0] * buffer.ndim
    start[dim] = index
    return lax.dynamic_update_slice(buffer, piece, start)


def both(mine, other, first, dim):
    low = jnp.where(first, mine, other)
    high = jnp.where(first, other, mine)
    return jnp.concatenate([low, high], axis=dim)


def gather_z(x, z, dim):
    half = x.shape[-2] // 2
    shape = list(x.shape)
    shape[dim] = 8
    out = put(jnp.zeros(shape, x.dtype), x, dim, z)
    up = down = x
    for k in range(1, 4):
        up, down = send(up, ZUP), send(down, ZDOWN)
        out = put(out, up, dim, (z - k) % 8)
        out = put(out, down, dim, (z + k) % 8)
    up = send(up[..., :half, :], ZUP)
    down = send(down[..., half:, :], ZDOWN)
    return put(out, jnp.concatenate([up, down], axis=-2), dim, (z + 4) % 8)


def local(rhs, coupling, diag_inverse):
    sec = lax.axis_index("sec")
    row = lax.axis_index("row")
    y, xl = sec // 2, sec % 2
    z, xh, core = row // 4, (row // 2) % 2, row % 2
    rows, total = rhs.shape
    width = diag_inverse.shape[1]
    half = width // 2
    cols = total // ROW
    low_x, low_h, low_core = xl == 0, xh == 0, core == 0

    slot = jnp.arange(width)
    i, rest = slot % rows, slot // rows
    natural = ((rest % 8) * 4 + ((rest // 8) % 2) * 2 + rest // 16) * rows + i
    pick = (jnp.arange(width)[:, None] == natural[None, :]).astype(BF)
    inverse = dot(diag_inverse[0], pick, NN).astype(BF)
    m = dot(coupling.reshape(SEC * rows, width), inverse, NN).astype(BF)
    m = m.reshape(SEC, rows, width)

    def blocks(first, count):
        return lax.dynamic_slice_in_dim(m, first, count, 0)

    far = lax.ppermute(m[6:8], "sec", [(0, 6), (1, 7)])
    next_pair = jnp.where(y == 3, far, blocks(jnp.minimum(2 * y + 2, 6), 2))
    away = lax.ppermute(blocks(5 + 2 * (y % 2), 1), "sec", [(s, s + 4) for s in range(4)])
    skip = jnp.where(y >= 2, away, blocks(4 + 2 * (y % 2), 1))
    inner = blocks(2 * y + 1, 1)
    given = lax.ppermute(inner[:, rows // 2 :], "sec", [(s, s + 1) for s in range(0, SEC, 2)])
    inner = jnp.where(low_x, inner[:, : rows // 2], given)

    wide = next_pair[:, None, None, None]
    wide = both(wide, send(wide, XL), low_x, 1)
    wide = both(wide, send(wide, XH), low_h, 2)
    near = gather_z(wide, z, 3).reshape(2, 2, half, width)
    mixed = jnp.concatenate([skip[0], inner[0]], axis=0)[None, None, None]
    mixed = gather_z(mixed, z, 2)
    mixed = both(mixed, send(mixed, XL), low_x, 0)
    mixed = both(mixed, send(mixed, XH), low_h, 1)
    jump = mixed[:, :, :, :rows].reshape(2, half, width)
    tied = jnp.moveaxis(mixed[:, :, :, rows:], 0, 2).reshape(half, width)

    lanes = rhs.T.reshape(8, 2, 2, cols, rows).transpose(2, 1, 0, 3, 4).reshape(ROW, cols, rows)
    mine = lax.all_to_all(lanes, BOTH, 0, 0, axis_index_groups=PLANES, tiled=True)
    mine = mine.reshape(2, 16, cols, rows).transpose(2, 0, 1, 3).reshape(cols, 2, half)

    def whole(part):
        return both(part, send(part, CORE), low_core, 1)

    def over_cores(part):
        part = part.astype(BF)
        return part.astype(F32) + send(part, CORE).astype(F32)

    def own_half(vector):
        return lax.dynamic_slice_in_dim(vector, core * half, half, vector.ndim - 1)

    def exchange(message):
        return lax.all_to_all(message, "sec", 0, 0, axis_index_groups=COLUMNS_Y, tiled=True)

    acc = jnp.zeros((cols, 2, half), F32)
    first = second = None
    for stage in range(4):
        resid = mine - acc
        top = whole(resid[:, 0].astype(BF))
        bottom = resid[:, 1] - dot(top, tied, NT)
        own = [top, whole(bottom.astype(BF))]
        if stage == 3:
            break
        if stage == 0:
            first = second = [jnp.zeros_like(top)] * 2
        from_near = [jnp.where(y == 3, a, b) for a, b in zip(first, own)]
        from_jump = [
            jnp.where(y < 2, c, jnp.where(y == 2, a, b)) for a, b, c in zip(first, second, own)
        ]
        to_next = [dot(from_near[0], near[t, 0], NT) + dot(from_near[1], near[t, 1], NT) for t in range(2)]
        to_jump = dot(from_jump[0], jump[0], NT) + dot(from_jump[1], jump[1], NT)
        target_next = jnp.minimum(y + 1, 3)
        target_jump = jnp.where(y % 2 == 0, 2, 3)
        out = []
        for q in range(4):
            parts = [jnp.where(target_next == q, p, 0.0) for p in to_next]
            for s in range(2):
                parts[s] = parts[s] + jnp.where((target_jump == q) & (y // 2 == s), to_jump, 0.0)
            out.append(jnp.concatenate([p.astype(BF) for p in parts] + own, axis=1))
        got = exchange(jnp.stack(out))
        acc = got[:, :, :width].astype(F32).sum(axis=0).reshape(cols, 2, half)
        first = [got[0, :, width : 2 * width], got[0, :, 2 * width :]]
        second = [got[1, :, width : 2 * width], got[1, :, 2 * width :]]

    keep = core == xl
    there = send(jnp.where(low_x, own[1], own[0]), XL)
    here = jnp.where(low_x, own[0], own[1])
    solved = dot(jnp.where(keep, here, there), inverse, NT)
    back = dot(solved.astype(BF), inverse, NN)
    back = both(back[:, None], send(back[:, None], XL), low_x, 1)
    back = jnp.where(keep, back, send(back, CORE))

    sent = jnp.zeros((cols, 2, width), F32)
    answer = None
    others = None
    for stage in range(4):
        mine_now = sent
        if stage > 0:
            above = jnp.where(y == 0, others[1], jnp.where(y == 1, others[2], others[3]))
            from_near = jnp.where(y == 3, halves, above)
            skipped = jnp.where(y == 0, others[2][:, 0], others[3][:, 0])
            from_jump = jnp.where(y < 2, skipped, halves[:, 1])
            by_near = [dot(from_near[:, 0], near[0, c], NN) + dot(from_near[:, 1], near[1, c], NN) for c in range(2)]
            by_jump = [dot(from_jump, jump[c], NN) for c in range(2)]
            by_near, by_jump = jnp.stack(by_near, 1), jnp.stack(by_jump, 1)
            mine_now = mine_now + jnp.where(y < 3, by_near, 0.0) + jnp.where(y < 2, by_jump, 0.0)
            target_0 = jnp.where(y == 3, by_near, 0.0) + jnp.where(y == 2, by_jump, 0.0)
            target_1 = jnp.where(y == 3, by_jump, 0.0)
            u = back - over_cores(mine_now)
        else:
            u = back
            target_0 = target_1 = jnp.zeros((cols, 2, width), F32)
        low = own_half(u[:, 1]).astype(BF)
        answer = jnp.stack([u[:, 0] - over_cores(dot(low, tied, NN)), u[:, 1]], axis=1)
        if stage == 3:
            break
        halves = own_half(answer).astype(BF)
        nothing = jnp.zeros((cols, 2 * width), BF)
        out = [
            jnp.concatenate([halves.reshape(cols, width), t], axis=1)
            for t in [
                target_0.astype(BF).reshape(cols, 2 * width),
                target_1.astype(BF).reshape(cols, 2 * width),
                nothing,
                nothing,
            ]
        ]
        got = exchange(jnp.stack(out))
        others = [got[q, :, :width].reshape(cols, 2, half) for q in range(4)]
        sent = got[:, :, width:].astype(F32).sum(axis=0).reshape(cols, 2, width)

    there = send(jnp.where(low_x, answer[:, 1], answer[:, 0]), XL)
    here = jnp.where(low_x, answer[:, 0], answer[:, 1])
    final = jnp.where(keep, here, there)
    final = final.reshape(cols, 2, 2, 8, rows).transpose(3, 2, 1, 0, 4).reshape(ROW, cols, rows)
    solved = solved.reshape(cols, ROW, rows).transpose(1, 0, 2)
    got = lax.all_to_all(jnp.concatenate([final, solved], axis=1), "row", 0, 0, tiled=True)
    got = got.reshape(ROW, 2, cols, rows).transpose(1, 3, 0, 2).reshape(2, rows, total)
    return (got[0], got[1])


def solution(mesh):
    return jax.shard_map(
        local,
        mesh=mesh,
        in_specs=(P(("sec", "row"), None), P(None, "row", "sec"), P("sec", None, None)),
        out_specs=(P(("sec", "row"), None), P(("sec", "row"), None)),
        check_vma=False,
    )
```

```python
import functools

import jax
import jax.numpy as jnp
from jax import lax
from jax.experimental import pallas as pl
from jax.experimental.pallas import tpu as pltpu
from jax.sharding import PartitionSpec as P

BF = jnp.bfloat16
F32 = jnp.float32
SEC, ROW = 8, 32
NT = (((1,), (1,)), ((), ()))
NN = (((1,), (0,)), ((), ()))
BOTH = ("sec", "row")


def place(dev):
    sec, row = divmod(dev, ROW)
    return sec // 2, sec % 2, row // 4, (row // 2) % 2, row % 2


def device(y, xl, z, xh, core):
    return (y * 2 + xl) * ROW + z * 4 + xh * 2 + core


def moved(move):
    return [(d, device(*move(*place(d)))) for d in range(SEC * ROW)]


XL = moved(lambda y, xl, z, xh, k: (y, 1 - xl, z, xh, k))
XH = moved(lambda y, xl, z, xh, k: (y, xl, z, 1 - xh, k))
CORE = moved(lambda y, xl, z, xh, k: (y, xl, z, xh, 1 - k))
ZUP = moved(lambda y, xl, z, xh, k: (y, xl, (z + 1) % 8, xh, k))
ZDOWN = moved(lambda y, xl, z, xh, k: (y, xl, (z - 1) % 8, xh, k))
YA = moved(lambda y, xl, z, xh, k: (y ^ 1, xl, z, xh, k))
YB = moved(lambda y, xl, z, xh, k: ({0: 3, 1: 2, 2: 1, 3: 0}[y], xl, z, xh, k))
PLANES = [
    [device(y, xl, z, xh, k) for xl in range(2) for xh in range(2) for z in range(8)]
    for y in range(4)
    for k in range(2)
]
SWAPS = [YA, YB, YA]


def send(x, pairs):
    return lax.ppermute(x, BOTH, pairs)


def dot(a, b, dims):
    return lax.dot_general(a, b, dims, preferred_element_type=F32)


def call(body, out, *args):
    specs = [pl.BlockSpec(memory_space=pltpu.SMEM)]
    specs += [pl.BlockSpec(memory_space=pltpu.VMEM)] * (len(args) - 1)
    many = isinstance(out, list)
    return pl.pallas_call(
        body,
        out_shape=out,
        in_specs=specs,
        out_specs=[pl.BlockSpec(memory_space=pltpu.VMEM)] * len(out) if many else pl.BlockSpec(memory_space=pltpu.VMEM),
        compiler_params=pltpu.CompilerParams(vmem_limit_bytes=20 * 2**20),
    )(*args)


def ring_z(x):
    part = x.shape[-2] // 2
    up = down = x
    ups, downs = [], []
    for _ in range(3):
        up, down = send(up, ZUP), send(down, ZDOWN)
        ups.append(up)
        downs.append(down)
    last = send(up[..., :part, :], ZUP), send(down[..., part:, :], ZDOWN)
    return [x, *ups, *downs, *last]


def lay_near(ids, *refs):
    out = refs[-1]
    xl, z, xh = ids[1], ids[2], ids[3]
    rows = refs[0].shape[2]
    part = rows // 2

    def lay(piece, at, first):
        for n in range(4):
            for t in range(2):
                start = ((xh + n // 2) % 2 * 8 + at % 8) * rows + first
                start = pl.multiple_of(start, part)
                out[t, (xl + n % 2) % 2, pl.ds(start, piece.shape[2]), :] = piece[n, t]

    for k in range(4):
        lay(refs[k], z + 8 - k, 0)
    for k in range(1, 4):
        lay(refs[3 + k], z + k, 0)
    lay(refs[7], z + 4, 0)
    lay(refs[8], z + 4, part)


def lay_plane(ids, *refs):
    out = refs[-1]
    z = ids[2]
    part = out.shape[-2] // 2
    for k in range(4):
        out[(z + 8 - k) % 8] = refs[k][...]
    for k in range(1, 4):
        out[(z + k) % 8] = refs[3 + k][...]
    out[(z + 4) % 8, :part] = refs[7][...]
    out[(z + 4) % 8, part:] = refs[8][...]


def lay_rest(ids, *refs):
    jump, tied = refs[-2:]
    xl, xh = ids[1], ids[3]
    part = refs[0].shape[1] // 3
    rows = 2 * part
    for n in range(4):
        at_l, at_h = (xl + n % 2) % 2, (xh + n // 2) % 2
        for z in range(8):
            start = pl.multiple_of((at_h * 8 + z) * rows, rows)
            jump[at_l, pl.ds(start, rows)] = refs[n][z, :rows]
            start = pl.multiple_of(start + at_l * part, part)
            tied[pl.ds(start, part)] = refs[n][z, rows:]


def wide(core, own, other, s, half):
    a, b = own[:, s * half : (s + 1) * half], other[:, s * half : (s + 1) * half]
    low = jnp.where(core == 0, a, b)
    high = jnp.where(core == 0, b, a)
    return jnp.concatenate([low, high], axis=1)


def forward_body(stage, ids, own, other, old, near, jump, tied, near_from, jump_from, *outs):
    y, core = ids[0], ids[4]
    half = own.shape[1] // 2
    width = 2 * half
    top = wide(core, own[...], other[...], 0, half).astype(BF)
    bottom = wide(core, own[...], other[...], 1, half) - dot(top, tied[...], NT)
    new = jnp.concatenate([top, bottom.astype(BF)], axis=1)
    kept = jnp.where(y == stage, new, old[...])
    outs[0][...] = kept
    if stage == 3:
        return
    source = kept if stage < 2 else jnp.where(y == 3, near_from[...], kept)
    for t in range(2):
        total = dot(source[:, :width], near[t, 0], NT) + dot(source[:, width:], near[t, 1], NT)
        outs[1][:, t * half : (t + 1) * half] = total
    source = kept if stage == 0 else jump_from[...]
    outs[1][:, width:] = dot(source[:, :width], jump[0], NT) + dot(source[:, width:], jump[1], NT)


def products_body(stage, ids, near_from, jump_from, near, jump, by_near, by_jump):
    half = near_from.shape[1] // 2
    width = 2 * half
    a, b = near_from[:, :half], near_from[:, half:]
    for c in range(2):
        by_near[:, c * width : (c + 1) * width] = dot(a, near[0, c], NN) + dot(b, near[1, c], NN)
        by_jump[:, c * width : (c + 1) * width] = dot(jump_from[...], jump[c], NN)


def solve_body(stage, ids, back, own, other, old, tied, jump, *outs):
    y, core = ids[0], ids[4]
    width = back.shape[1] // 2
    half = width // 2
    u = back[...] - (own[...].astype(F32) + other[...].astype(F32))
    x1 = u[:, width:]
    x0 = u[:, :width] - dot(x1.astype(BF), tied[...], NN)
    kept = jnp.where(y == 3 - stage, jnp.concatenate([x0, x1], axis=1), old[...])
    outs[0][...] = kept
    if stage == 3:
        return
    parts = [
        jnp.where(core == 0, kept[:, s * width : s * width + half], kept[:, s * width + half : (s + 1) * width])
        for s in range(2)
    ]
    outs[1][...] = jnp.concatenate(parts, axis=1).astype(BF)
    if stage == 0:
        for c in range(2):
            outs[2][:, c * width : (c + 1) * width] = dot(parts[1].astype(BF), jump[c], NN)


def local(rhs, coupling, diag_inverse):
    sec = lax.axis_index("sec")
    row = lax.axis_index("row")
    y, xl = sec // 2, sec % 2
    z, xh, core = row // 4, (row // 2) % 2, row % 2
    ids = jnp.stack([y, xl, z, xh, core]).astype(jnp.int32)
    rows, total = rhs.shape
    width = diag_inverse.shape[1]
    half = width // 2
    cols = total // ROW

    slot = jnp.arange(width)
    i, rest = slot % rows, slot // rows
    natural = ((rest % 8) * 4 + ((rest // 8) % 2) * 2 + rest // 16) * rows + i
    pick = (jnp.arange(width)[:, None] == natural[None, :]).astype(BF)
    inverse = dot(diag_inverse[0], pick, NN).astype(BF)
    m = dot(coupling.reshape(SEC * rows, width), inverse, NN).astype(BF)
    m = m.reshape(SEC, rows, width)

    def blocks(first, count):
        return lax.dynamic_slice_in_dim(m, first, count, 0)

    far = lax.ppermute(m[6:8], "sec", [(0, 6), (1, 7), (2, 4), (3, 5)])
    close = lax.ppermute(blocks(5 + 2 * (y % 2), 1), "sec", [(0, 2), (1, 3), (2, 6), (3, 7)])
    inner = blocks(2 * y + 1, 1)[0]
    given = lax.ppermute(inner[rows // 2 :], "sec", [(s, s + 1) for s in range(0, SEC, 2)])
    next_pair = jnp.where(y == 3, far, blocks(jnp.minimum(2 * y + 2, 6), 2))
    skip = jnp.where(y == 0, m[4], jnp.where(y == 2, far[0], close[0]))
    inner = jnp.where(xl == 0, inner[: rows // 2], given)

    beside = send(next_pair, XL)
    across = send(jnp.stack([next_pair, beside]), XH)
    near = ring_z(jnp.stack([next_pair, beside, across[0], across[1]]))
    near = call(lay_near, pltpu.VMEM((2, 2, half, width), BF), ids, *near)

    mixed = ring_z(jnp.concatenate([skip, inner], axis=0))
    mixed = call(lay_plane, jax.ShapeDtypeStruct((8, *mixed[0].shape), BF), ids, *mixed)
    beside = send(mixed, XL)
    rest = [mixed, beside, send(mixed, XH), send(beside, XH)]
    shapes = [
        pltpu.VMEM((2, half, width), BF),
        jax.ShapeDtypeStruct((half, width), BF),
    ]
    jump, tied = call(lay_rest, shapes, ids, *rest)
    other = send(tied, CORE)
    tied = jnp.concatenate([jnp.where(core == 0, tied, other), jnp.where(core == 0, other, tied)], axis=0)

    lanes = rhs.T.reshape(8, 2, 2, cols, rows).transpose(2, 1, 0, 3, 4).reshape(ROW, cols * rows // 128, 128)
    mine = lax.all_to_all(lanes, BOTH, 0, 0, axis_index_groups=PLANES, tiled=True)
    mine = mine.reshape(2, 16, cols, rows).transpose(2, 0, 1, 3).reshape(cols, width)

    def struct(n, dtype):
        return jax.ShapeDtypeStruct((cols, n), dtype)

    zero_z = jnp.zeros((cols, 2 * width), BF)
    kept, got_z, resid, stash, ours = zero_z, zero_z, mine, None, None
    for stage in range(4):
        shapes = [struct(2 * width, BF)] + ([struct(width + half, F32)] if stage < 3 else [])
        got = call(
            functools.partial(forward_body, stage), shapes, ids, resid, send(resid, CORE), kept, near, jump, tied, got_z, got_z
        )
        kept = got[0]
        if stage == 3:
            break
        update, leap = got[1][:, :width], got[1][:, width:]
        if stage == 0:
            sent = jnp.concatenate([update.astype(BF), leap.astype(BF), kept], axis=1)
        elif stage == 1:
            update = update + jnp.concatenate([stash.astype(F32), leap], axis=1)
            sent = jnp.concatenate([update.astype(BF), kept], axis=1)
        else:
            ours = update
            update = update + jnp.concatenate([leap, jnp.zeros_like(leap)], axis=1)
            sent = jnp.concatenate([update.astype(BF), got_z], axis=1)
        arrived = send(sent, SWAPS[stage])
        acc, got_z = arrived[:, :width].astype(F32), arrived[:, -2 * width :]
        if stage == 0:
            stash = arrived[:, width : width + half]
        if stage == 2:
            late = dot(got_z[:, :width], jump[0], NT) + dot(got_z[:, width:], jump[1], NT)
            acc = acc + ours + jnp.concatenate([jnp.zeros_like(late), late], axis=1)
        resid = mine - acc

    def mine_of(pair):
        low, high = pair[:, :width], pair[:, width:]
        there = send(jnp.where(xl == 0, high, low), XL)
        return jnp.where(core == xl, jnp.where(xl == 0, low, high), there)

    solved = dot(mine_of(kept), inverse, NT)
    back = dot(solved.astype(BF), inverse, NN)
    there = send(back, XL)
    back = jnp.concatenate([jnp.where(xl == 0, back, there), jnp.where(xl == 0, there, back)], axis=1)
    back = jnp.where(core == xl, back, send(back, CORE))

    zero = jnp.zeros((cols, 2 * width), F32)
    answer, halves, own, other = zero, None, zero.astype(BF), zero.astype(BF)
    arrived, ours = None, None
    for stage in range(4):
        if stage > 0:
            got_x = arrived[:, :width]
            got_c = arrived[:, width : 3 * width].astype(F32)
            if stage == 1:
                sources = jnp.where(y == 3, halves, got_x), got_x[:, :half]
            elif stage == 2:
                sources = got_x, got_x[:, half:]
            else:
                sources = got_x, arrived[:, 3 * width :]
            by_near, by_jump = call(
                functools.partial(products_body, stage), [struct(2 * width, F32)] * 2, ids, *sources, near, jump
            )
            if stage == 1:
                own = by_near
                give = jnp.where(y == 3, by_near, by_jump + got_c)
            elif stage == 2:
                own, ours, give = by_near + got_c, got_c, by_jump
            else:
                own = by_near + by_jump + got_c + ours
            own = own.astype(BF)
            other = send(own, CORE)
        shapes = [struct(2 * width, F32)]
        shapes += [struct(width, BF)] if stage < 3 else []
        shapes += [struct(2 * width, F32)] if stage == 0 else []
        got = call(functools.partial(solve_body, stage), shapes, ids, back, own, other, answer, tied, jump)
        answer = got[0]
        if stage == 3:
            break
        halves = got[1]
        if stage == 0:
            give = got[2]
        sent = [halves, give.astype(BF)] + ([got_x[:, :half]] if stage == 2 else [])
        arrived = send(jnp.concatenate(sent, axis=1), SWAPS[stage])

    final = mine_of(answer)
    final = final.reshape(cols, 2, 2, 8, rows).transpose(3, 2, 1, 0, 4).reshape(ROW, cols * rows // 128, 128)
    solved = solved.reshape(cols, ROW, rows).transpose(1, 0, 2).reshape(ROW, cols * rows // 128, 128)
    got = lax.all_to_all(jnp.concatenate([final, solved], axis=1), "row", 0, 0, tiled=True)
    got = got.reshape(ROW, 2, cols, rows).transpose(1, 3, 0, 2).reshape(2, rows, total)
    return (got[0], got[1])


def solution(mesh):
    return jax.shard_map(
        local,
        mesh=mesh,
        in_specs=(P(("sec", "row"), None), P(None, "row", "sec"), P("sec", None, None)),
        out_specs=(P(("sec", "row"), None), P(("sec", "row"), None)),
        check_vma=False,
    )
```

```python
import functools

import jax
import jax.numpy as jnp
from jax import lax
from jax.experimental import pallas as pl
from jax.experimental.pallas import tpu as pltpu
from jax.sharding import PartitionSpec as P


BF = jnp.bfloat16
F32 = jnp.float32
SEC, ROW = 8, 32
NT = (((1,), (1,)), ((), ()))
NN = (((1,), (0,)), ((), ()))
BOTH = ("sec", "row")


def place(dev):
    sec, row = divmod(dev, ROW)
    return sec // 2, sec % 2, row // 4, (row // 2) % 2, row % 2


def device(y, xl, z, xh, core):
    return (y * 2 + xl) * ROW + z * 4 + xh * 2 + core


def moved(move):
    return [(d, device(*move(*place(d)))) for d in range(SEC * ROW)]


XL = moved(lambda y, xl, z, xh, k: (y, 1 - xl, z, xh, k))
XH = moved(lambda y, xl, z, xh, k: (y, xl, z, 1 - xh, k))
CORE = moved(lambda y, xl, z, xh, k: (y, xl, z, xh, 1 - k))
ZUP = moved(lambda y, xl, z, xh, k: (y, xl, (z + 1) % 8, xh, k))
ZDOWN = moved(lambda y, xl, z, xh, k: (y, xl, (z - 1) % 8, xh, k))
YA = moved(lambda y, xl, z, xh, k: (y ^ 1, xl, z, xh, k))
YB = moved(lambda y, xl, z, xh, k: ({0: 3, 1: 2, 2: 1, 3: 0}[y], xl, z, xh, k))
PLANES = [
    [device(y, xl, z, xh, k) for xl in range(2) for xh in range(2) for z in range(8)]
    for y in range(4)
    for k in range(2)
]
SWAPS = [YA, YB, YA]


def send(x, pairs):
    return lax.ppermute(x, BOTH, pairs)


def dot(a, b, dims):
    return lax.dot_general(a, b, dims, preferred_element_type=F32)


def call(body, out, *args, copies=0):
    specs = [pl.BlockSpec(memory_space=pltpu.SMEM)]
    specs += [pl.BlockSpec(memory_space=pl.ANY if copies else pltpu.VMEM)] * (len(args) - 1)
    many = isinstance(out, list)
    return pl.pallas_call(
        body,
        out_shape=out,
        in_specs=specs,
        out_specs=[pl.BlockSpec(memory_space=pltpu.VMEM)] * len(out) if many else pl.BlockSpec(memory_space=pltpu.VMEM),
        scratch_shapes=[pltpu.SemaphoreType.DMA((copies,))] if copies else [],
        compiler_params=pltpu.CompilerParams(vmem_limit_bytes=20 * 2**20),
    )(*args)


def ring_z(x):
    part = x.shape[-2] // 2
    up = down = x
    ups, downs = [], []
    for _ in range(1, 4):
        up, down = send(up, ZUP), send(down, ZDOWN)
        ups.append(up)
        downs.append(down)
    last = send(up[..., :part, :], ZUP), send(down[..., part:, :], ZDOWN)
    return [x, *ups, *downs, *last]


def run_copies(pairs, sems):
    copies = [pltpu.make_async_copy(src, dst, sems.at[n]) for n, (src, dst) in enumerate(pairs)]
    for copy in copies:
        copy.start()
    for copy in copies:
        copy.wait()


def lay_near(ids, *refs):
    out, sems = refs[-2:]
    xl, z, xh = ids[1], ids[2], ids[3]
    rows = refs[0].shape[2]
    part = rows // 2
    pairs = []

    def lay(piece, at, first):
        for n in range(4):
            for t in range(2):
                start = ((xh + n // 2) % 2 * 8 + at % 8) * rows + first
                start = pl.multiple_of(start, part)
                pairs.append((piece.at[n, t], out.at[t, (xl + n % 2) % 2, pl.ds(start, piece.shape[2])]))

    for k in range(4):
        lay(refs[k], z + 8 - k, 0)
    for k in range(1, 4):
        lay(refs[3 + k], z + k, 0)
    lay(refs[7], z + 4, 0)
    lay(refs[8], z + 4, part)
    run_copies(pairs, sems)


def lay_plane(ids, *refs):
    out = refs[-1]
    z = ids[2]
    part = out.shape[-2] // 2
    for k in range(4):
        out[(z + 8 - k) % 8] = refs[k][...]
    for k in range(1, 4):
        out[(z + k) % 8] = refs[3 + k][...]
    out[(z + 4) % 8, :part] = refs[7][...]
    out[(z + 4) % 8, part:] = refs[8][...]


def lay_rest(ids, *refs):
    jump, tied, sems = refs[-3:]
    xl, xh = ids[1], ids[3]
    part = refs[0].shape[1] // 3
    rows = 2 * part
    pairs = []
    for n in range(4):
        at_l, at_h = (xl + n % 2) % 2, (xh + n // 2) % 2
        for z in range(8):
            start = pl.multiple_of((at_h * 8 + z) * rows, rows)
            pairs.append((refs[n].at[z, :rows], jump.at[at_l, pl.ds(start, rows)]))
            start = pl.multiple_of(start + at_l * part, part)
            pairs.append((refs[n].at[z, rows:], tied.at[pl.ds(start, part)]))
    run_copies(pairs, sems)


def lay_tied(ids, own, other, out, sems):
    half = own.shape[0]
    start = pl.multiple_of(ids[4] * half, half)
    end = pl.multiple_of((1 - ids[4]) * half, half)
    run_copies([(own, out.at[pl.ds(start, half)]), (other, out.at[pl.ds(end, half)])], sems)


def wide(core, own, other, s, half):
    a, b = own[:, s * half : (s + 1) * half], other[:, s * half : (s + 1) * half]
    low = jnp.where(core == 0, a, b)
    high = jnp.where(core == 0, b, a)
    return jnp.concatenate([low, high], axis=1)


def forward_body(stage, ids, own, other, old, near, jump, tied, near_from, jump_from, *outs):
    y, core = ids[0], ids[4]
    half = own.shape[1] // 2
    width = 2 * half
    top = wide(core, own[...], other[...], 0, half).astype(BF)
    bottom = wide(core, own[...], other[...], 1, half) - dot(top, tied[...], NT)
    new = jnp.concatenate([top, bottom.astype(BF)], axis=1)
    kept = jnp.where(y == stage, new, old[...])
    outs[0][...] = kept
    if stage == 3:
        return
    source = kept if stage < 2 else jnp.where(y == 3, near_from[...], kept)
    for t in range(2):
        total = dot(source[:, :width], near[t, 0], NT) + dot(source[:, width:], near[t, 1], NT)
        outs[1][:, t * half : (t + 1) * half] = total
    source = kept if stage == 0 else jump_from[...]
    outs[1][:, width:] = dot(source[:, :width], jump[0], NT) + dot(source[:, width:], jump[1], NT)


def products_body(ids, near_from, jump_from, near, jump, by_near, by_jump):
    half = near_from.shape[1] // 2
    width = 2 * half
    a, b = near_from[:, :half], near_from[:, half:]
    for c in range(2):
        by_near[:, c * width : (c + 1) * width] = dot(a, near[0, c], NN) + dot(b, near[1, c], NN)
        by_jump[:, c * width : (c + 1) * width] = dot(jump_from[...], jump[c], NN)


def solve_body(stage, ids, back, own, other, old, tied, jump, *outs):
    y, core = ids[0], ids[4]
    width = back.shape[1] // 2
    half = width // 2
    u = back[...] - (own[...].astype(F32) + other[...].astype(F32))
    x1 = u[:, width:]
    x0 = u[:, :width] - dot(x1.astype(BF), tied[...], NN)
    kept = jnp.where(y == 3 - stage, jnp.concatenate([x0, x1], axis=1), old[...])
    outs[0][...] = kept
    if stage == 3:
        return
    parts = [
        jnp.where(core == 0, kept[:, s * width : s * width + half], kept[:, s * width + half : (s + 1) * width])
        for s in range(2)
    ]
    outs[1][...] = jnp.concatenate(parts, axis=1).astype(BF)
    if stage == 0:
        for c in range(2):
            outs[2][:, c * width : (c + 1) * width] = dot(parts[1].astype(BF), jump[c], NN)


def solve(rhs, coupling, diag_inverse):
    sec = lax.axis_index("sec")
    row = lax.axis_index("row")
    y, xl = sec // 2, sec % 2
    z, xh, core = row // 4, (row // 2) % 2, row % 2
    ids = jnp.stack([y, xl, z, xh, core]).astype(jnp.int32)
    rows, total = rhs.shape
    width = diag_inverse.shape[1]
    half = width // 2
    cols = total // ROW

    slot = jnp.arange(width)
    i, rest = slot % rows, slot // rows
    natural = ((rest % 8) * 4 + ((rest // 8) % 2) * 2 + rest // 16) * rows + i
    pick = (jnp.arange(width)[:, None] == natural[None, :]).astype(BF)
    inverse = dot(diag_inverse[0], pick, NN).astype(BF)
    m = dot(coupling.reshape(SEC * rows, width), inverse, NN).astype(BF)
    m = m.reshape(SEC, rows, width)

    def blocks(first, count):
        return lax.dynamic_slice_in_dim(m, first, count, 0)

    far = lax.ppermute(m[6:8], "sec", [(0, 6), (1, 7), (2, 4), (3, 5)])
    close = lax.ppermute(blocks(5 + 2 * (y % 2), 1), "sec", [(0, 2), (1, 3), (2, 6), (3, 7)])
    inner = blocks(2 * y + 1, 1)[0]
    given = lax.ppermute(inner[rows // 2 :], "sec", [(s, s + 1) for s in range(0, SEC, 2)])
    next_pair = jnp.where(y == 3, far, blocks(jnp.minimum(2 * y + 2, 6), 2))
    skip = jnp.where(y == 0, m[4], jnp.where(y == 2, far[0], close[0]))
    inner = jnp.where(xl == 0, inner[: rows // 2], given)

    beside = send(next_pair, XL)
    across = send(jnp.stack([next_pair, beside]), XH)
    near = ring_z(jnp.stack([next_pair, beside, across[0], across[1]]))
    near = call(lay_near, pltpu.VMEM((2, 2, half, width), BF), ids, *near, copies=72)

    mixed = ring_z(jnp.concatenate([skip, inner], axis=0))
    mixed = call(lay_plane, jax.ShapeDtypeStruct((8, *mixed[0].shape), BF), ids, *mixed)
    beside = send(mixed, XL)
    rest = [mixed, beside, send(mixed, XH), send(beside, XH)]
    shapes = [pltpu.VMEM((2, half, width), BF), jax.ShapeDtypeStruct((half, width), BF)]
    jump, tied = call(lay_rest, shapes, ids, *rest, copies=64)
    tied = call(lay_tied, pltpu.VMEM((width, width), BF), ids, tied, send(tied, CORE), copies=2)

    lanes = rhs.T.reshape(8, 2, 2, cols, rows).transpose(2, 1, 0, 3, 4).reshape(ROW, cols * rows // 128, 128)
    mine = lax.all_to_all(lanes, BOTH, 0, 0, axis_index_groups=PLANES, tiled=True)
    mine = mine.reshape(2, 16, cols, rows).transpose(2, 0, 1, 3).reshape(cols, width)

    def struct(n, dtype):
        return jax.ShapeDtypeStruct((cols, n), dtype)

    zero_z = jnp.zeros((cols, 2 * width), BF)
    kept, got_z, resid, stash, ours = zero_z, zero_z, mine, None, None
    for stage in range(4):
        shapes = [struct(2 * width, BF)] + ([struct(width + half, F32)] if stage < 3 else [])
        got = call(
            functools.partial(forward_body, stage), shapes, ids, resid, send(resid, CORE), kept, near, jump, tied, got_z, got_z
        )
        kept = got[0]
        if stage == 3:
            break
        update, leap = got[1][:, :width], got[1][:, width:]
        if stage == 0:
            sent = jnp.concatenate([update.astype(BF), leap.astype(BF), kept], axis=1)
        elif stage == 1:
            update = update + jnp.concatenate([stash.astype(F32), leap], axis=1)
            sent = jnp.concatenate([update.astype(BF), kept], axis=1)
        else:
            ours = update
            update = update + jnp.concatenate([leap, jnp.zeros_like(leap)], axis=1)
            sent = jnp.concatenate([update.astype(BF), got_z], axis=1)
        arrived = send(sent, SWAPS[stage])
        acc, got_z = arrived[:, :width].astype(F32), arrived[:, -2 * width :]
        if stage == 0:
            stash = arrived[:, width : width + half]
        if stage == 2:
            late = dot(got_z[:, :width], jump[0], NT) + dot(got_z[:, width:], jump[1], NT)
            acc = acc + ours + jnp.concatenate([jnp.zeros_like(late), late], axis=1)
        resid = mine - acc

    def mine_of(pair):
        low, high = pair[:, :width], pair[:, width:]
        there = send(jnp.where(xl == 0, high, low), XL)
        return jnp.where(core == xl, jnp.where(xl == 0, low, high), there)

    solved = dot(mine_of(kept), inverse, NT)
    back = dot(solved.astype(BF), inverse, NN)
    there = send(back, XL)
    back = jnp.concatenate([jnp.where(xl == 0, back, there), jnp.where(xl == 0, there, back)], axis=1)
    back = jnp.where(core == xl, back, send(back, CORE))

    zero = jnp.zeros((cols, 2 * width), F32)
    answer, halves, own, other = zero, None, zero.astype(BF), zero.astype(BF)
    arrived, ours = None, None
    for stage in range(4):
        if stage > 0:
            got_x = arrived[:, :width]
            got_c = arrived[:, width : 3 * width].astype(F32)
            if stage == 1:
                sources = jnp.where(y == 3, halves, got_x), got_x[:, :half]
            elif stage == 2:
                sources = got_x, got_x[:, half:]
            else:
                sources = got_x, arrived[:, 3 * width :]
            by_near, by_jump = call(products_body, [struct(2 * width, F32)] * 2, ids, *sources, near, jump)
            if stage == 1:
                own = by_near
                give = jnp.where(y == 3, by_near, by_jump + got_c)
            elif stage == 2:
                own, ours, give = by_near + got_c, got_c, by_jump
            else:
                own = by_near + by_jump + got_c + ours
            own = own.astype(BF)
            other = send(own, CORE)
        shapes = [struct(2 * width, F32)]
        shapes += [struct(width, BF)] if stage < 3 else []
        shapes += [struct(2 * width, F32)] if stage == 0 else []
        got = call(functools.partial(solve_body, stage), shapes, ids, back, own, other, answer, tied, jump)
        answer = got[0]
        if stage == 3:
            break
        halves = got[1]
        if stage == 0:
            give = got[2]
        sent = [halves, give.astype(BF)] + ([got_x[:, :half]] if stage == 2 else [])
        arrived = send(jnp.concatenate(sent, axis=1), SWAPS[stage])

    final = mine_of(answer)
    final = final.reshape(cols, 2, 2, 8, rows).transpose(3, 2, 1, 0, 4).reshape(ROW, cols * rows // 128, 128)
    solved = solved.reshape(cols, ROW, rows).transpose(1, 0, 2).reshape(ROW, cols * rows // 128, 128)
    got = lax.all_to_all(jnp.concatenate([final, solved], axis=1), "row", 0, 0, tiled=True)
    got = got.reshape(ROW, 2, cols, rows).transpose(1, 3, 0, 2).reshape(2, rows, total)
    return (got[0], got[1])


def solution(mesh):
    return jax.shard_map(
        solve,
        mesh=mesh,
        in_specs=(P(("sec", "row"), None), P(None, "row", "sec"), P("sec", None, None)),
        out_specs=(P(("sec", "row"), None), P(("sec", "row"), None)),
        check_vma=False,
    )
```

```python
import functools

import jax
import jax.numpy as jnp
from jax import lax
from jax.experimental import pallas as pl
from jax.experimental.pallas import tpu as pltpu
from jax.sharding import PartitionSpec as P


BF = jnp.bfloat16
F32 = jnp.float32
SEC, ROW = 8, 32
NT = (((1,), (1,)), ((), ()))
NN = (((1,), (0,)), ((), ()))
BOTH = ("sec", "row")


def place(dev):
    sec, row = divmod(dev, ROW)
    return sec // 2, sec % 2, row // 4, (row // 2) % 2, row % 2


def device(y, xl, z, xh, core):
    return (y * 2 + xl) * ROW + z * 4 + xh * 2 + core


def moved(move):
    return [(d, device(*move(*place(d)))) for d in range(SEC * ROW)]


XL = moved(lambda y, xl, z, xh, k: (y, 1 - xl, z, xh, k))
XH = moved(lambda y, xl, z, xh, k: (y, xl, z, 1 - xh, k))
CORE = moved(lambda y, xl, z, xh, k: (y, xl, z, xh, 1 - k))
ZUP = moved(lambda y, xl, z, xh, k: (y, xl, (z + 1) % 8, xh, k))
ZDOWN = moved(lambda y, xl, z, xh, k: (y, xl, (z - 1) % 8, xh, k))
XP = moved(lambda y, xl, z, xh, k: (y, 1 - xl, z, (xh + xl) % 2, k))
XM = moved(lambda y, xl, z, xh, k: (y, 1 - xl, z, (xh + 1 - xl) % 2, k))
YA = moved(lambda y, xl, z, xh, k: (y ^ 1, xl, z, xh, k))
YB = moved(lambda y, xl, z, xh, k: ({0: 3, 1: 2, 2: 1, 3: 0}[y], xl, z, xh, k))
PLANES = [
    [device(y, xl, z, xh, k) for xl in range(2) for xh in range(2) for z in range(8)]
    for y in range(4)
    for k in range(2)
]
SWAPS = [YA, YB, YA]


def send(x, pairs):
    return lax.ppermute(x, BOTH, pairs)


def dot(a, b, dims):
    return lax.dot_general(a, b, dims, preferred_element_type=F32)


def call(body, out, *args):
    specs = [pl.BlockSpec(memory_space=pltpu.SMEM)]
    specs += [pl.BlockSpec(memory_space=pltpu.VMEM)] * (len(args) - 1)
    many = isinstance(out, list)
    return pl.pallas_call(
        body,
        out_shape=out,
        in_specs=specs,
        out_specs=[pl.BlockSpec(memory_space=pltpu.VMEM)] * len(out) if many else pl.BlockSpec(memory_space=pltpu.VMEM),
        compiler_params=pltpu.CompilerParams(vmem_limit_bytes=20 * 2**20),
    )(*args)


def ring_z(x):
    part = x.shape[-2] // 7 * 4
    up = down = x
    ups, downs = [], []
    for _ in range(1, 4):
        up, down = send(up, ZUP), send(down, ZDOWN)
        ups.append(up)
        downs.append(down)
    last = send(up[..., :part, :], ZUP), send(down[..., part:, :], ZDOWN)
    return [x, *ups, *downs, *last]


def lay_all(ids, *refs):
    near, jump, tied = refs[-3:]
    z, x = ids[2], ids[3] * 2 + ids[1]
    total = refs[0].shape[1]
    part = total // 7
    rows = 2 * part
    for piece, offset, first in zip(refs[:9], [0, 7, 6, 5, 1, 2, 3, 4, 4], [0] * 8 + [4 * part]):
        at_z = (z + offset) % 8
        for n, dx in enumerate([0, 3, 1, 2]):
            at_x = (x + dx) % 4
            xl, xh = at_x % 2, at_x // 2
            start = pl.multiple_of((xh * 8 + at_z) * rows, rows)
            for block in range(piece.shape[1] // part):
                number = first // part + block
                from_rows = slice(block * part, (block + 1) * part)
                shift = number % 2 * part
                if number < 4:
                    near[number // 2, xl, pl.ds(pl.multiple_of(start + shift, part), part)] = piece[n, from_rows]
                elif number < 6:
                    jump[xl, pl.ds(pl.multiple_of(start + shift, part), part)] = piece[n, from_rows]
                else:
                    tied[pl.ds(pl.multiple_of(start + xl * part, part), part)] = piece[n, from_rows]


def lay_tied(ids, own, other, out):
    half = own.shape[0]
    out[pl.ds(pl.multiple_of(ids[4] * half, half), half)] = own[...]
    out[pl.ds(pl.multiple_of((1 - ids[4]) * half, half), half)] = other[...]


def wide(core, own, other, s, half):
    a, b = own[:, s * half : (s + 1) * half], other[:, s * half : (s + 1) * half]
    low = jnp.where(core == 0, a, b)
    high = jnp.where(core == 0, b, a)
    return jnp.concatenate([low, high], axis=1)


def forward_body(stage, ids, own, other, old, near, jump, tied, near_from, jump_from, *outs):
    y, core = ids[0], ids[4]
    half = own.shape[1] // 2
    width = 2 * half
    top = wide(core, own[...], other[...], 0, half).astype(BF)
    bottom = wide(core, own[...], other[...], 1, half) - dot(top, tied[...], NT)
    new = jnp.concatenate([top, bottom.astype(BF)], axis=1)
    kept = jnp.where(y == stage, new, old[...])
    outs[0][...] = kept
    if stage == 3:
        return
    source = kept if stage < 2 else jnp.where(y == 3, near_from[...], kept)
    for t in range(2):
        total = dot(source[:, :width], near[t, 0], NT) + dot(source[:, width:], near[t, 1], NT)
        outs[1][:, t * half : (t + 1) * half] = total
    source = kept if stage == 0 else jump_from[...]
    outs[1][:, width:] = dot(source[:, :width], jump[0], NT) + dot(source[:, width:], jump[1], NT)


def products_body(ids, near_from, jump_from, near, jump, by_near, by_jump):
    half = near_from.shape[1] // 2
    width = 2 * half
    a, b = near_from[:, :half], near_from[:, half:]
    for c in range(2):
        by_near[:, c * width : (c + 1) * width] = dot(a, near[0, c], NN) + dot(b, near[1, c], NN)
        by_jump[:, c * width : (c + 1) * width] = dot(jump_from[...], jump[c], NN)


def solve_body(stage, ids, back, own, other, old, tied, jump, *outs):
    y, core = ids[0], ids[4]
    width = back.shape[1] // 2
    half = width // 2
    u = back[...] - (own[...].astype(F32) + other[...].astype(F32))
    x1 = u[:, width:]
    x0 = u[:, :width] - dot(x1.astype(BF), tied[...], NN)
    kept = jnp.where(y == 3 - stage, jnp.concatenate([x0, x1], axis=1), old[...])
    outs[0][...] = kept
    if stage == 3:
        return
    parts = [
        jnp.where(core == 0, kept[:, s * width : s * width + half], kept[:, s * width + half : (s + 1) * width])
        for s in range(2)
    ]
    outs[1][...] = jnp.concatenate(parts, axis=1).astype(BF)
    if stage == 0:
        for c in range(2):
            outs[2][:, c * width : (c + 1) * width] = dot(parts[1].astype(BF), jump[c], NN)


def solve(rhs, coupling, diag_inverse):
    sec = lax.axis_index("sec")
    row = lax.axis_index("row")
    y, xl = sec // 2, sec % 2
    z, xh, core = row // 4, (row // 2) % 2, row % 2
    ids = jnp.stack([y, xl, z, xh, core]).astype(jnp.int32)
    rows, total = rhs.shape
    width = diag_inverse.shape[1]
    half = width // 2
    cols = total // ROW

    slot = jnp.arange(width)
    i, rest = slot % rows, slot // rows
    natural = ((rest % 8) * 4 + ((rest // 8) % 2) * 2 + rest // 16) * rows + i
    pick = (jnp.arange(width)[:, None] == natural[None, :]).astype(BF)
    inverse = dot(diag_inverse[0], pick, NN).astype(BF)
    m = dot(coupling.reshape(SEC * rows, width), inverse, NN).astype(BF)
    m = m.reshape(SEC, rows, width)

    def blocks(first, count):
        return lax.dynamic_slice_in_dim(m, first, count, 0)

    far = send(m[6:8], YB)
    close = lax.ppermute(blocks(5 + 2 * (y % 2), 1), "sec", [(0, 2), (1, 3), (2, 6), (3, 7)])
    inner = blocks(2 * y + 1, 1)[0]
    given = send(inner[rows // 2 :], XL)
    next_pair = jnp.where(y == 3, far, blocks(jnp.minimum(2 * y + 2, 6), 2))
    skip = jnp.where(y == 0, m[4], jnp.where(y == 2, far[0], close[0]))
    inner = jnp.where(xl == 0, inner[: rows // 2], given)

    lanes = rhs.T.reshape(8, 2, 2, cols, rows).transpose(2, 1, 0, 3, 4).reshape(ROW, cols * rows // 128, 128)
    mine = lax.all_to_all(lanes, BOTH, 0, 0, axis_index_groups=PLANES, tiled=True)
    mine = mine.reshape(2, 16, cols, rows).transpose(2, 0, 1, 3).reshape(cols, width)

    unit = jnp.concatenate([next_pair.reshape(2 * rows, width), skip, inner], axis=0)
    pieces = ring_z(jnp.stack([unit, send(unit, XP), send(unit, XM), send(unit, XH)]))
    pieces = [pltpu.with_memory_space_constraint(p, pltpu.VMEM) for p in pieces]
    shapes = [pltpu.VMEM((2, 2, half, width), BF), pltpu.VMEM((2, half, width), BF), pltpu.VMEM((half, width), BF)]
    keep = core == xl
    early = jnp.where(keep, jnp.ones((8, 128), F32), 0.0)
    near, jump, tied = call(lay_all, shapes, ids, *pieces, mine, early)
    tied = call(lay_tied, pltpu.VMEM((width, width), BF), ids, tied, send(tied, CORE))

    def struct(n, dtype):
        return jax.ShapeDtypeStruct((cols, n), dtype)

    zero_z = jnp.zeros((cols, 2 * width), BF)
    kept, got_z, resid, stash, ours = zero_z, zero_z, mine, None, None
    for stage in range(4):
        shapes = [struct(2 * width, BF)] + ([struct(width + half, F32)] if stage < 3 else [])
        got = call(
            functools.partial(forward_body, stage), shapes, ids, resid, send(resid, CORE), kept, near, jump, tied, got_z, got_z
        )
        kept = got[0]
        if stage == 3:
            break
        update, leap = got[1][:, :width], got[1][:, width:]
        if stage == 0:
            sent = jnp.concatenate([update.astype(BF), leap.astype(BF), kept], axis=1)
        elif stage == 1:
            update = update + jnp.concatenate([stash.astype(F32), leap], axis=1)
            sent = jnp.concatenate([update.astype(BF), kept], axis=1)
        else:
            ours = update
            update = update + jnp.concatenate([leap, jnp.zeros_like(leap)], axis=1)
            sent = jnp.concatenate([update.astype(BF), got_z], axis=1)
        arrived = send(sent, SWAPS[stage])
        acc, got_z = arrived[:, :width].astype(F32), arrived[:, -2 * width :]
        if stage == 0:
            stash = arrived[:, width : width + half]
        if stage == 2:
            late = dot(got_z[:, :width], jump[0], NT) + dot(got_z[:, width:], jump[1], NT)
            acc = acc + ours + jnp.concatenate([jnp.zeros_like(late), late], axis=1)
        resid = mine - acc

    def mine_of(pair):
        low, high = pair[:, :width], pair[:, width:]
        there = send(jnp.where(xl == 0, high, low), XL)
        return jnp.where(keep, jnp.where(xl == 0, low, high), there)

    solved = dot(mine_of(kept), inverse, NT)
    back = dot(solved.astype(BF), inverse, NN)
    there = send(back, XL)
    back = jnp.concatenate([jnp.where(xl == 0, back, there), jnp.where(xl == 0, there, back)], axis=1)
    back = jnp.where(keep, back, send(back, CORE))

    zero = jnp.zeros((cols, 2 * width), F32)
    answer, halves, own, other = zero, None, zero.astype(BF), zero.astype(BF)
    arrived, ours = None, None
    for stage in range(4):
        if stage > 0:
            got_x = arrived[:, :width]
            got_c = arrived[:, width : 3 * width].astype(F32)
            if stage == 1:
                sources = jnp.where(y == 3, halves, got_x), got_x[:, :half]
            elif stage == 2:
                sources = got_x, got_x[:, half:]
            else:
                sources = got_x, arrived[:, 3 * width :]
            by_near, by_jump = call(products_body, [struct(2 * width, F32)] * 2, ids, *sources, near, jump)
            if stage == 1:
                own = by_near
                give = jnp.where(y == 3, by_near, by_jump + got_c)
            elif stage == 2:
                own, ours, give = by_near + got_c, got_c, by_jump
            else:
                own = by_near + by_jump + got_c + ours
            own = own.astype(BF)
            other = send(own, CORE)
        shapes = [struct(2 * width, F32)]
        shapes += [struct(width, BF)] if stage < 3 else []
        shapes += [struct(2 * width, F32)] if stage == 0 else []
        got = call(functools.partial(solve_body, stage), shapes, ids, back, own, other, answer, tied, jump)
        answer = got[0]
        if stage == 3:
            break
        halves = got[1]
        if stage == 0:
            give = got[2]
        sent = [halves, give.astype(BF)] + ([got_x[:, :half]] if stage == 2 else [])
        arrived = send(jnp.concatenate(sent, axis=1), SWAPS[stage])

    final = mine_of(answer)
    final = final.reshape(cols, 2, 2, 8, rows).transpose(3, 2, 1, 0, 4).reshape(ROW, cols * rows // 128, 128)
    solved = solved.reshape(cols, ROW, rows).transpose(1, 0, 2).reshape(ROW, cols * rows // 128, 128)
    got = lax.all_to_all(jnp.concatenate([final, solved], axis=1), "row", 0, 0, tiled=True)
    got = got.reshape(ROW, 2, cols, rows).transpose(1, 3, 0, 2).reshape(2, rows, total)
    return (got[0], got[1])


def solution(mesh):
    return jax.shard_map(
        solve,
        mesh=mesh,
        in_specs=(P(("sec", "row"), None), P(None, "row", "sec"), P("sec", None, None)),
        out_specs=(P(("sec", "row"), None), P(("sec", "row"), None)),
        check_vma=False,
    )
```

```python
import functools

import jax
import jax.numpy as jnp
from jax import lax
from jax.experimental import pallas as pl
from jax.experimental.pallas import tpu as pltpu
from jax.sharding import PartitionSpec as P


BF = jnp.bfloat16
F32 = jnp.float32
SEC, ROW = 8, 32
NT = (((1,), (1,)), ((), ()))
NN = (((1,), (0,)), ((), ()))
BOTH = ("sec", "row")


def place(dev):
    sec, row = divmod(dev, ROW)
    return sec // 2, sec % 2, row // 4, (row // 2) % 2, row % 2


def device(y, xl, z, xh, core):
    return (y * 2 + xl) * ROW + z * 4 + xh * 2 + core


def moved(move):
    return [(d, device(*move(*place(d)))) for d in range(SEC * ROW)]


XL = moved(lambda y, xl, z, xh, k: (y, 1 - xl, z, xh, k))
XH = moved(lambda y, xl, z, xh, k: (y, xl, z, 1 - xh, k))
CORE = moved(lambda y, xl, z, xh, k: (y, xl, z, xh, 1 - k))
ZUP = moved(lambda y, xl, z, xh, k: (y, xl, (z + 1) % 8, xh, k))
ZDOWN = moved(lambda y, xl, z, xh, k: (y, xl, (z - 1) % 8, xh, k))
XP = moved(lambda y, xl, z, xh, k: (y, 1 - xl, z, (xh + xl) % 2, k))
XM = moved(lambda y, xl, z, xh, k: (y, 1 - xl, z, (xh + 1 - xl) % 2, k))
CROSS = moved(lambda y, xl, z, xh, k: (y, k, z, xh, xl))
YA = moved(lambda y, xl, z, xh, k: (y ^ 1, xl, z, xh, k))
YB = moved(lambda y, xl, z, xh, k: ({0: 3, 1: 2, 2: 1, 3: 0}[y], xl, z, xh, k))
PLANES = [
    [device(y, xl, z, xh, k) for xl in range(2) for xh in range(2) for z in range(8)]
    for y in range(4)
    for k in range(2)
]
RINGS = [
    [device(y, xl, z, xh, k) for z in range(8)] for y in range(4) for xl in range(2) for xh in range(2) for k in range(2)
]
SWAPS = [YA, YB, YA]


def send(x, pairs):
    return lax.ppermute(x, BOTH, pairs)


def dot(a, b, dims):
    return lax.dot_general(a, b, dims, preferred_element_type=F32)


def call(body, out, *args):
    specs = [pl.BlockSpec(memory_space=pltpu.SMEM)]
    specs += [pl.BlockSpec(memory_space=pltpu.VMEM)] * (len(args) - 1)
    many = isinstance(out, list)
    return pl.pallas_call(
        body,
        out_shape=out,
        in_specs=specs,
        out_specs=[pl.BlockSpec(memory_space=pltpu.VMEM)] * len(out) if many else pl.BlockSpec(memory_space=pltpu.VMEM),
        compiler_params=pltpu.CompilerParams(vmem_limit_bytes=20 * 2**20),
    )(*args)


def ring_z(x):
    part = x.shape[-2] // 5 * 3
    up = down = x
    ups, downs = [], []
    for _ in range(1, 4):
        up, down = send(up, ZUP), send(down, ZDOWN)
        ups.append(up)
        downs.append(down)
    last = send(up[..., :part, :], ZUP), send(down[..., part:, :], ZDOWN)
    return [x, *ups, *downs, *last]


def lay_all(ids, *refs):
    near, jump, tied = refs[-3:]
    z, x = ids[2], ids[3] * 2 + ids[1]
    part = refs[0].shape[1] // 5
    rows = 2 * part

    def spot(n, at_z):
        at_x = (x + [0, 3, 1, 2][n]) % 4
        return at_x % 2, pl.multiple_of((at_x // 2 * 8 + at_z) * rows, rows)

    for piece, offset, first in zip(refs[:9], [0, 7, 6, 5, 1, 2, 3, 4, 4], [0] * 8 + [3]):
        for n in range(4):
            xl, start = spot(n, (z + offset) % 8)
            for block in range(piece.shape[1] // part):
                number = first + block
                rows_in = slice(block * part, (block + 1) * part)
                if number < 4:
                    begin = pl.multiple_of(start + number % 2 * part, part)
                    near[number // 2, xl, pl.ds(begin, part)] = piece[n, rows_in]
                else:
                    tied[pl.ds(pl.multiple_of(start + xl * part, part), part)] = piece[n, rows_in]
    for n, plane in enumerate(refs[9:13]):
        for at_z in range(8):
            xl, start = spot(n, at_z)
            jump[xl, pl.ds(start, rows)] = plane[at_z]


def lay_tied(ids, own, other, out):
    half = own.shape[0]
    out[pl.ds(pl.multiple_of(ids[4] * half, half), half)] = own[...]
    out[pl.ds(pl.multiple_of((1 - ids[4]) * half, half), half)] = other[...]


def wide(core, own, other, s, half):
    a, b = own[:, s * half : (s + 1) * half], other[:, s * half : (s + 1) * half]
    low = jnp.where(core == 0, a, b)
    high = jnp.where(core == 0, b, a)
    return jnp.concatenate([low, high], axis=1)


def forward_body(stage, ids, own, other, old, near, jump, tied, near_from, jump_from, *outs):
    y, core = ids[0], ids[4]
    half = own.shape[1] // 2
    width = 2 * half
    top = wide(core, own[...], other[...], 0, half).astype(BF)
    bottom = wide(core, own[...], other[...], 1, half) - dot(top, tied[...], NT)
    new = jnp.concatenate([top, bottom.astype(BF)], axis=1)
    kept = jnp.where(y == stage, new, old[...])
    outs[0][...] = kept
    if stage == 3:
        return
    source = kept if stage < 2 else jnp.where(y == 3, near_from[...], kept)
    for t in range(2):
        total = dot(source[:, :width], near[t, 0], NT) + dot(source[:, width:], near[t, 1], NT)
        outs[1][:, t * half : (t + 1) * half] = total
    source = kept if stage == 0 else jump_from[...]
    outs[1][:, width:] = dot(source[:, :width], jump[0], NT) + dot(source[:, width:], jump[1], NT)


def products_body(ids, near_from, jump_from, near, jump, by_near, by_jump):
    half = near_from.shape[1] // 2
    width = 2 * half
    a, b = near_from[:, :half], near_from[:, half:]

    def column(c, carry):
        at = pl.ds(pl.multiple_of(c * width, width), width)
        by_near[:, at] = dot(a, near[0, c], NN) + dot(b, near[1, c], NN)
        by_jump[:, at] = dot(jump_from[...], jump[c], NN)
        return carry

    lax.fori_loop(0, 2, column, 0)


def solve_body(stage, ids, back, own, other, old, tied, jump, *outs):
    y, core = ids[0], ids[4]
    width = back.shape[1] // 2
    half = width // 2
    u = back[...] - (own[...].astype(F32) + other[...].astype(F32))
    x1 = u[:, width:]
    x0 = u[:, :width] - dot(x1.astype(BF), tied[...], NN)
    kept = jnp.where(y == 3 - stage, jnp.concatenate([x0, x1], axis=1), old[...])
    outs[0][...] = kept
    if stage == 3:
        return
    parts = [
        jnp.where(core == 0, kept[:, s * width : s * width + half], kept[:, s * width + half : (s + 1) * width])
        for s in range(2)
    ]
    outs[1][...] = jnp.concatenate(parts, axis=1).astype(BF)
    if stage == 0:
        for c in range(2):
            outs[2][:, c * width : (c + 1) * width] = dot(parts[1].astype(BF), jump[c], NN)


def solve(rhs, coupling, diag_inverse):
    sec = lax.axis_index("sec")
    row = lax.axis_index("row")
    y, xl = sec // 2, sec % 2
    z, xh, core = row // 4, (row // 2) % 2, row % 2
    ids = jnp.stack([y, xl, z, xh, core]).astype(jnp.int32)
    rows, total = rhs.shape
    width = diag_inverse.shape[1]
    half = width // 2
    cols = total // ROW

    slot = jnp.arange(width)
    i, rest = slot % rows, slot // rows
    natural = ((rest % 8) * 4 + ((rest // 8) % 2) * 2 + rest // 16) * rows + i
    pick = (jnp.arange(width)[:, None] == natural[None, :]).astype(BF)
    inverse = dot(diag_inverse[0], pick, NN).astype(BF)
    m = dot(coupling.reshape(SEC * rows, width), inverse, NN).astype(BF)
    m = m.reshape(SEC, rows, width)

    def blocks(first, count):
        return lax.dynamic_slice_in_dim(m, first, count, 0)

    far = send(m[6:8], YB)
    close = lax.ppermute(blocks(5 + 2 * (y % 2), 1), "sec", [(0, 2), (1, 3), (2, 6), (3, 7)])
    inner = blocks(2 * y + 1, 1)[0]
    given = send(inner[rows // 2 :], XL)
    next_pair = jnp.where(y == 3, far, blocks(jnp.minimum(2 * y + 2, 6), 2))
    skip = jnp.where(y == 0, m[4], jnp.where(y == 2, far[0], close[0]))
    inner = jnp.where(xl == 0, inner[: rows // 2], given)

    lanes = rhs.T.reshape(8, 2, 2, cols, rows).transpose(2, 1, 0, 3, 4).reshape(ROW, cols * rows // 128, 128)
    mine = lax.all_to_all(lanes, BOTH, 0, 0, axis_index_groups=PLANES, tiled=True)
    mine = mine.reshape(2, 16, cols, rows).transpose(2, 0, 1, 3).reshape(cols, width)

    unit = jnp.concatenate([next_pair.reshape(2 * rows, width), inner], axis=0)
    unit = jnp.stack([unit, send(unit, XP), send(unit, XM), send(unit, XH)])
    plane = lax.all_to_all(jnp.broadcast_to(skip, (8, rows, width)), BOTH, 0, 0, axis_index_groups=RINGS, tiled=True)
    planes = [plane, send(plane, XP), send(plane, XM), send(plane, XH)]
    pieces = ring_z(unit) + planes
    pieces = [pltpu.with_memory_space_constraint(p, pltpu.VMEM) for p in pieces]
    shapes = [pltpu.VMEM((2, 2, half, width), BF), pltpu.VMEM((2, half, width), BF), pltpu.VMEM((half, width), BF)]
    away = send(inverse, [(a, b) for a, b in CROSS if a != b])
    inverse = jnp.where(core == xl, inverse, away)
    early = jnp.where(core == 0, jnp.ones((8, 128), F32), 0.0)
    near, jump, tied = call(lay_all, shapes, ids, *pieces, mine, inverse, early)
    tied = call(lay_tied, pltpu.VMEM((width, width), BF), ids, tied, send(tied, CORE))

    def struct(n, dtype):
        return jax.ShapeDtypeStruct((cols, n), dtype)

    zero_z = jnp.zeros((cols, 2 * width), BF)
    kept, got_z, resid, stash, ours = zero_z, zero_z, mine, None, None
    for stage in range(4):
        shapes = [struct(2 * width, BF)] + ([struct(width + half, F32)] if stage < 3 else [])
        got = call(
            functools.partial(forward_body, stage), shapes, ids, resid, send(resid, CORE), kept, near, jump, tied, got_z, got_z
        )
        kept = got[0]
        if stage == 3:
            break
        update, leap = got[1][:, :width], got[1][:, width:]
        if stage == 0:
            sent = jnp.concatenate([update.astype(BF), leap.astype(BF), kept], axis=1)
        elif stage == 1:
            update = update + jnp.concatenate([stash.astype(F32), leap], axis=1)
            sent = jnp.concatenate([update.astype(BF), kept], axis=1)
        else:
            ours = update
            update = update + jnp.concatenate([leap, jnp.zeros_like(leap)], axis=1)
            sent = jnp.concatenate([update.astype(BF), got_z], axis=1)
        arrived = send(sent, SWAPS[stage])
        acc, got_z = arrived[:, :width].astype(F32), arrived[:, -2 * width :]
        if stage == 0:
            stash = arrived[:, width : width + half]
        if stage == 2:
            late = dot(got_z[:, :width], jump[0], NT) + dot(got_z[:, width:], jump[1], NT)
            acc = acc + ours + jnp.concatenate([jnp.zeros_like(late), late], axis=1)
        resid = mine - acc

    def mine_of(pair):
        return jnp.where(core == 0, pair[:, :width], pair[:, width:])

    solved = dot(mine_of(kept), inverse, NT)
    back = dot(solved.astype(BF), inverse, NN)
    other = send(back, CORE)
    back = jnp.concatenate([jnp.where(core == 0, back, other), jnp.where(core == 0, other, back)], axis=1)

    zero = jnp.zeros((cols, 2 * width), F32)
    answer, halves, own, other = zero, None, zero.astype(BF), zero.astype(BF)
    arrived, ours = None, None
    for stage in range(4):
        if stage > 0:
            got_x = arrived[:, :width]
            got_c = arrived[:, width : 3 * width].astype(F32)
            if stage == 1:
                sources = jnp.where(y == 3, halves, got_x), got_x[:, :half]
            elif stage == 2:
                sources = got_x, got_x[:, half:]
            else:
                sources = got_x, arrived[:, 3 * width :]
            by_near, by_jump = call(products_body, [struct(2 * width, F32)] * 2, ids, *sources, near, jump)
            if stage == 1:
                own = by_near
                give = jnp.where(y == 3, by_near, by_jump + got_c)
            elif stage == 2:
                own, ours, give = by_near + got_c, got_c, by_jump
            else:
                own = by_near + by_jump + got_c + ours
            own = own.astype(BF)
            other = send(own, CORE)
        shapes = [struct(2 * width, F32)]
        shapes += [struct(width, BF)] if stage < 3 else []
        shapes += [struct(2 * width, F32)] if stage == 0 else []
        got = call(functools.partial(solve_body, stage), shapes, ids, back, own, other, answer, tied, jump)
        answer = got[0]
        if stage == 3:
            break
        halves = got[1]
        if stage == 0:
            give = got[2]
        sent = [halves, give.astype(BF)] + ([got_x[:, :half]] if stage == 2 else [])
        arrived = send(jnp.concatenate(sent, axis=1), SWAPS[stage])

    final = send(jnp.concatenate([mine_of(answer), solved], axis=1).astype(BF), CROSS)
    solved = final[:, width:].reshape(cols, ROW, rows).transpose(1, 0, 2)
    final = final[:, :width].reshape(cols, 2, 2, 8, rows).transpose(3, 2, 1, 0, 4).reshape(ROW, cols, rows)
    final = jnp.concatenate([final, solved], axis=1).reshape(ROW, 2 * cols * rows // 128, 128)
    got = lax.all_to_all(final, "row", 0, 0, tiled=True).astype(F32)
    got = got.reshape(ROW, 2, cols, rows).transpose(1, 3, 0, 2).reshape(2, rows, total)
    return (got[0], got[1])


def solution(mesh):
    return jax.shard_map(
        solve,
        mesh=mesh,
        in_specs=(P(("sec", "row"), None), P(None, "row", "sec"), P("sec", None, None)),
        out_specs=(P(("sec", "row"), None), P(("sec", "row"), None)),
        check_vma=False,
    )
```

```python
import functools

import jax
import jax.numpy as jnp
from jax import lax
from jax.experimental import pallas as pl
from jax.experimental.pallas import tpu as pltpu
from jax.sharding import PartitionSpec as P


BF = jnp.bfloat16
F32 = jnp.float32
SEC, ROW = 8, 32
NT = (((1,), (1,)), ((), ()))
NN = (((1,), (0,)), ((), ()))
BOTH = ("sec", "row")


def place(dev):
    sec, row = divmod(dev, ROW)
    return sec // 2, sec % 2, row // 4, (row // 2) % 2, row % 2


def device(y, xl, z, xh, core):
    return (y * 2 + xl) * ROW + z * 4 + xh * 2 + core


def moved(move):
    return [(d, device(*move(*place(d)))) for d in range(SEC * ROW)]


XL = moved(lambda y, xl, z, xh, k: (y, 1 - xl, z, xh, k))
XH = moved(lambda y, xl, z, xh, k: (y, xl, z, 1 - xh, k))
CORE = moved(lambda y, xl, z, xh, k: (y, xl, z, xh, 1 - k))
ZUP = moved(lambda y, xl, z, xh, k: (y, xl, (z + 1) % 8, xh, k))
ZDOWN = moved(lambda y, xl, z, xh, k: (y, xl, (z - 1) % 8, xh, k))
XP = moved(lambda y, xl, z, xh, k: (y, 1 - xl, z, (xh + xl) % 2, k))
XM = moved(lambda y, xl, z, xh, k: (y, 1 - xl, z, (xh + 1 - xl) % 2, k))
CROSS = moved(lambda y, xl, z, xh, k: (y, k, z, xh, xl))
YA = moved(lambda y, xl, z, xh, k: (y ^ 1, xl, z, xh, k))
YB = moved(lambda y, xl, z, xh, k: ({0: 3, 1: 2, 2: 1, 3: 0}[y], xl, z, xh, k))
PLANES = [
    [device(y, xl, z, xh, k) for xl in range(2) for xh in range(2) for z in range(8)]
    for y in range(4)
    for k in range(2)
]
RINGS = [
    [device(y, xl, z, xh, k) for z in range(8)] for y in range(4) for xl in range(2) for xh in range(2) for k in range(2)
]
SWAPS = [YA, YB, YA]


def send(x, pairs):
    return lax.ppermute(x, BOTH, pairs)


def dot(a, b, dims):
    return lax.dot_general(a, b, dims, preferred_element_type=F32)


def call(body, out, *args):
    specs = [pl.BlockSpec(memory_space=pltpu.SMEM)]
    specs += [pl.BlockSpec(memory_space=pltpu.VMEM)] * (len(args) - 1)
    many = isinstance(out, list)
    return pl.pallas_call(
        body,
        out_shape=out,
        in_specs=specs,
        out_specs=[pl.BlockSpec(memory_space=pltpu.VMEM)] * len(out) if many else pl.BlockSpec(memory_space=pltpu.VMEM),
        compiler_params=pltpu.CompilerParams(vmem_limit_bytes=20 * 2**20),
    )(*args)


def ring_z(x):
    part = x.shape[-2] // 5 * 3
    up = down = x
    ups, downs = [], []
    for _ in range(1, 4):
        up, down = send(up, ZUP), send(down, ZDOWN)
        ups.append(up)
        downs.append(down)
    last = send(up[..., :part, :], ZUP), send(down[..., part:, :], ZDOWN)
    return [x, *ups, *downs, *last]


def lay_all(ids, *refs):
    near, jump, tied = refs[-3:]
    z, x = ids[2], ids[3] * 2 + ids[1]
    part = refs[0].shape[1] // 5
    rows = 2 * part

    def spot(n, at_z):
        at_x = (x + [0, 3, 1, 2][n]) % 4
        return at_x % 2, pl.multiple_of((at_x // 2 * 8 + at_z) * rows, rows)

    for piece, offset, first in zip(refs[:9], [0, 7, 6, 5, 1, 2, 3, 4, 4], [0] * 8 + [3]):
        for n in range(4):
            xl, start = spot(n, (z + offset) % 8)
            for block in range(piece.shape[1] // part):
                number = first + block
                rows_in = slice(block * part, (block + 1) * part)
                if number < 4:
                    begin = pl.multiple_of(start + number % 2 * part, part)
                    near[number // 2, xl, pl.ds(begin, part)] = piece[n, rows_in]
                else:
                    tied[pl.ds(pl.multiple_of(start + xl * part, part), part)] = piece[n, rows_in]
    for n, plane in enumerate(refs[9:13]):
        for at_z in range(8):
            xl, start = spot(n, at_z)
            jump[xl, pl.ds(start, rows)] = plane[at_z]


def lay_tied(ids, own, other, out):
    half = own.shape[0]
    out[pl.ds(pl.multiple_of(ids[4] * half, half), half)] = own[...]
    out[pl.ds(pl.multiple_of((1 - ids[4]) * half, half), half)] = other[...]


def wide(core, own, other, s, half):
    a, b = own[:, s * half : (s + 1) * half], other[:, s * half : (s + 1) * half]
    low = jnp.where(core == 0, a, b)
    high = jnp.where(core == 0, b, a)
    return jnp.concatenate([low, high], axis=1)


def forward_body(stage, ids, own, other, old, near, jump, tied, near_from, *outs):
    y, core = ids[0], ids[4]
    half = own.shape[1] // 2
    width = 2 * half
    top = wide(core, own[...], other[...], 0, half).astype(BF)
    bottom = wide(core, own[...], other[...], 1, half) - dot(top, tied[...], NT)
    new = jnp.concatenate([top, bottom.astype(BF)], axis=1)
    kept = jnp.where(y == stage, new, old[...])
    outs[0][...] = kept
    if stage == 3:
        return
    source = kept if stage < 2 else jnp.where(y == 3, near_from[...], kept)

    def section(t, carry):
        total = dot(source[:, :width], near[t, 0], NT) + dot(source[:, width:], near[t, 1], NT)
        outs[1][:, pl.ds(pl.multiple_of(t * half, half), half)] = total
        return carry

    lax.fori_loop(0, 2, section, 0)
    if stage == 0:
        outs[1][:, width:] = dot(kept[:, :width], jump[0], NT) + dot(kept[:, width:], jump[1], NT)


def near_body(ids, source, near, out):
    half = source.shape[1] // 2
    width = 2 * half
    a, b = source[:, :half], source[:, half:]

    def column(c, carry):
        at = pl.ds(pl.multiple_of(c * width, width), width)
        out[:, at] = dot(a, near[0, c], NN) + dot(b, near[1, c], NN)
        return carry

    lax.fori_loop(0, 2, column, 0)


def jump_body(ids, source, jump, out):
    width = jump.shape[2]

    def column(c, carry):
        out[:, pl.ds(pl.multiple_of(c * width, width), width)] = dot(source[...], jump[c], NN)
        return carry

    lax.fori_loop(0, 2, column, 0)


def solve_body(stage, ids, back, own, other, old, tied, jump, *outs):
    y, core = ids[0], ids[4]
    width = back.shape[1] // 2
    half = width // 2
    u = back[...] - (own[...].astype(F32) + other[...].astype(F32))
    x1 = u[:, width:]
    x0 = u[:, :width] - dot(x1.astype(BF), tied[...], NN)
    kept = jnp.where(y == 3 - stage, jnp.concatenate([x0, x1], axis=1), old[...])
    outs[0][...] = kept
    if stage == 3:
        return
    parts = [
        jnp.where(core == 0, kept[:, s * width : s * width + half], kept[:, s * width + half : (s + 1) * width])
        for s in range(2)
    ]
    outs[1][...] = jnp.concatenate(parts, axis=1).astype(BF)
    if stage == 0:
        for c in range(2):
            outs[2][:, c * width : (c + 1) * width] = dot(parts[1].astype(BF), jump[c], NN)


def solve(rhs, coupling, diag_inverse):
    sec = lax.axis_index("sec")
    row = lax.axis_index("row")
    y, xl = sec // 2, sec % 2
    z, xh, core = row // 4, (row // 2) % 2, row % 2
    ids = jnp.stack([y, xl, z, xh, core]).astype(jnp.int32)
    rows, total = rhs.shape
    width = diag_inverse.shape[1]
    half = width // 2
    cols = total // ROW

    slot = jnp.arange(width)
    i, rest = slot % rows, slot // rows
    natural = ((rest % 8) * 4 + ((rest // 8) % 2) * 2 + rest // 16) * rows + i
    pick = (jnp.arange(width)[:, None] == natural[None, :]).astype(BF)
    m = dot(coupling.reshape(SEC * rows, width), diag_inverse[0], NN).astype(BF)
    m = dot(m, pick, NN).astype(BF).reshape(SEC, rows, width)
    inverse = dot(diag_inverse[0], pick, NN).astype(BF)

    def blocks(first, count):
        return lax.dynamic_slice_in_dim(m, first, count, 0)

    far = send(m[6:8], YB)
    inner = blocks(2 * y + 1, 1)[0]
    given = send(inner[rows // 2 :], XL)
    close = lax.ppermute(blocks(5 + 2 * (y % 2), 1), "sec", [(0, 2), (1, 3), (2, 6), (3, 7)])
    next_pair = jnp.where(y == 3, far, blocks(jnp.minimum(2 * y + 2, 6), 2))
    skip = jnp.where(y == 0, m[4], jnp.where(y == 2, far[0], close[0]))
    inner = jnp.where(xl == 0, inner[: rows // 2], given)

    lanes = rhs.T.reshape(8, 2, 2, cols, rows).transpose(2, 1, 0, 3, 4).reshape(ROW, cols * rows // 128, 128)
    mine = lax.all_to_all(lanes, BOTH, 0, 0, axis_index_groups=PLANES, tiled=True)
    mine = mine.reshape(2, 16, cols, rows).transpose(2, 0, 1, 3).reshape(cols, width)

    unit = jnp.concatenate([next_pair.reshape(2 * rows, width), inner], axis=0)
    unit = jnp.stack([unit, send(unit, XP), send(unit, XM), send(unit, XH)])
    plane = lax.all_to_all(jnp.broadcast_to(skip, (8, rows, width)), BOTH, 0, 0, axis_index_groups=RINGS, tiled=True)
    planes = [plane, send(plane, XP), send(plane, XM), send(plane, XH)]
    pieces = ring_z(unit) + planes
    pieces = [pltpu.with_memory_space_constraint(p, pltpu.VMEM) for p in pieces]
    shapes = [pltpu.VMEM((2, 2, half, width), BF), pltpu.VMEM((2, half, width), BF), pltpu.VMEM((half, width), BF)]
    away = send(inverse, [(a, b) for a, b in CROSS if a != b])
    inverse = jnp.where(core == xl, inverse, away)
    early = jnp.where(core == 0, jnp.ones((8, 128), F32), 0.0)
    near, jump, tied = call(lay_all, shapes, ids, *pieces, mine, inverse, early)
    tied = call(lay_tied, pltpu.VMEM((width, width), BF), ids, tied, send(tied, CORE))

    def struct(n, dtype):
        return jax.ShapeDtypeStruct((cols, n), dtype)

    zero_z = jnp.zeros((cols, 2 * width), BF)
    kept, got_z, resid, stash, ours = zero_z, zero_z, mine, None, None
    for stage in range(4):
        shapes = [struct(2 * width, BF)]
        shapes += [struct(width + half if stage == 0 else width, F32)] if stage < 3 else []
        across = send(resid, CORE)
        if 0 < stage < 3:
            leap = dot(got_z[:, :width], jump[0], NT) + dot(got_z[:, width:], jump[1], NT)
        got = call(functools.partial(forward_body, stage), shapes, ids, resid, across, kept, near, jump, tied, got_z)
        kept = got[0]
        if stage == 3:
            break
        update = got[1][:, :width]
        if stage == 0:
            leap = got[1][:, width:]
        if stage == 0:
            sent = jnp.concatenate([update.astype(BF), leap.astype(BF), kept], axis=1)
        elif stage == 1:
            update = update + jnp.concatenate([stash.astype(F32), leap], axis=1)
            sent = jnp.concatenate([update.astype(BF), kept], axis=1)
        else:
            ours = update
            update = update + jnp.concatenate([leap, jnp.zeros_like(leap)], axis=1)
            sent = jnp.concatenate([update.astype(BF), got_z], axis=1)
        arrived = send(sent, SWAPS[stage])
        acc, got_z = arrived[:, :width].astype(F32), arrived[:, -2 * width :]
        if stage == 0:
            stash = arrived[:, width : width + half]
        if stage == 2:
            late = dot(got_z[:, :width], jump[0], NT) + dot(got_z[:, width:], jump[1], NT)
            acc = acc + ours + jnp.concatenate([jnp.zeros_like(late), late], axis=1)
        resid = mine - acc

    def mine_of(pair):
        return jnp.where(core == 0, pair[:, :width], pair[:, width:])

    solved = dot(mine_of(kept), inverse, NT)
    back = dot(solved.astype(BF), inverse, NN)
    other = send(back, CORE)
    back = jnp.concatenate([jnp.where(core == 0, back, other), jnp.where(core == 0, other, back)], axis=1)

    zero = jnp.zeros((cols, 2 * width), F32)
    answer, halves, own, other = zero, None, zero.astype(BF), zero.astype(BF)
    arrived, ours = None, None
    for stage in range(4):
        if stage > 0:
            got_x = arrived[:, :width]
            got_c = arrived[:, width : 3 * width].astype(F32)
            if stage == 1:
                sources = jnp.where(y == 3, halves, got_x), got_x[:, :half]
            elif stage == 2:
                sources = got_x, got_x[:, half:]
            else:
                sources = got_x, arrived[:, 3 * width :]
            by_near = call(near_body, struct(2 * width, F32), ids, sources[0], near)
            by_jump = call(jump_body, struct(2 * width, F32), ids, sources[1], jump)
            if stage == 1:
                own = by_near
                give = jnp.where(y == 3, by_near, by_jump + got_c)
            elif stage == 2:
                own, ours, give = by_near + got_c, got_c, by_jump
            else:
                own = by_near + by_jump + got_c + ours
            own = own.astype(BF)
            other = send(own, CORE)
        shapes = [struct(2 * width, F32)]
        shapes += [struct(width, BF)] if stage < 3 else []
        shapes += [struct(2 * width, F32)] if stage == 0 else []
        got = call(functools.partial(solve_body, stage), shapes, ids, back, own, other, answer, tied, jump)
        answer = got[0]
        if stage == 3:
            break
        halves = got[1]
        if stage == 0:
            give = got[2]
        sent = [halves, give.astype(BF)] + ([got_x[:, :half]] if stage == 2 else [])
        arrived = send(jnp.concatenate(sent, axis=1), SWAPS[stage])

    final = send(jnp.concatenate([mine_of(answer), solved], axis=1).astype(BF), CROSS)
    solved = final[:, width:].reshape(cols, ROW, rows).transpose(1, 0, 2)
    final = final[:, :width].reshape(cols, 2, 2, 8, rows).transpose(3, 2, 1, 0, 4).reshape(ROW, cols, rows)
    final = jnp.concatenate([final, solved], axis=1).reshape(ROW, 2 * cols * rows // 128, 128)
    got = lax.all_to_all(final, "row", 0, 0, tiled=True).astype(F32)
    got = got.reshape(ROW, 2, cols, rows).transpose(1, 3, 0, 2).reshape(2, rows, total)
    return (got[0], got[1])


def solution(mesh):
    return jax.shard_map(
        solve,
        mesh=mesh,
        in_specs=(P(("sec", "row"), None), P(None, "row", "sec"), P("sec", None, None)),
        out_specs=(P(("sec", "row"), None), P(("sec", "row"), None)),
        check_vma=False,
    )
```

```python
import functools

import jax
import jax.numpy as jnp
from jax import lax
from jax.experimental import pallas as pl
from jax.experimental.pallas import tpu as pltpu
from jax.sharding import PartitionSpec as P


BF = jnp.bfloat16
F32 = jnp.float32
SEC, ROW = 8, 32
NT = (((1,), (1,)), ((), ()))
NN = (((1,), (0,)), ((), ()))
BOTH = ("sec", "row")


def place(dev):
    sec, row = divmod(dev, ROW)
    return sec // 2, sec % 2, row // 4, (row // 2) % 2, row % 2


def device(y, xl, z, xh, core):
    return (y * 2 + xl) * ROW + z * 4 + xh * 2 + core


def moved(move):
    return [(d, device(*move(*place(d)))) for d in range(SEC * ROW)]


XL = moved(lambda y, xl, z, xh, k: (y, 1 - xl, z, xh, k))
XH = moved(lambda y, xl, z, xh, k: (y, xl, z, 1 - xh, k))
CORE = moved(lambda y, xl, z, xh, k: (y, xl, z, xh, 1 - k))
ZUP = moved(lambda y, xl, z, xh, k: (y, xl, (z + 1) % 8, xh, k))
ZDOWN = moved(lambda y, xl, z, xh, k: (y, xl, (z - 1) % 8, xh, k))
XP = moved(lambda y, xl, z, xh, k: (y, 1 - xl, z, (xh + xl) % 2, k))
XM = moved(lambda y, xl, z, xh, k: (y, 1 - xl, z, (xh + 1 - xl) % 2, k))
CROSS = moved(lambda y, xl, z, xh, k: (y, k, z, xh, xl))
YA = moved(lambda y, xl, z, xh, k: (y ^ 1, xl, z, xh, k))
YB = moved(lambda y, xl, z, xh, k: ({0: 3, 1: 2, 2: 1, 3: 0}[y], xl, z, xh, k))
PLANES = [
    [device(y, xl, z, xh, k) for xl in range(2) for xh in range(2) for z in range(8)]
    for y in range(4)
    for k in range(2)
]
RINGS = [
    [device(y, xl, z, xh, k) for z in range(8)] for y in range(4) for xl in range(2) for xh in range(2) for k in range(2)
]
SWAPS = [YA, YB, YA]


def send(x, pairs):
    return lax.ppermute(x, BOTH, pairs)


def dot(a, b, dims):
    return lax.dot_general(a, b, dims, preferred_element_type=F32)


def call(body, out, *args):
    specs = [pl.BlockSpec(memory_space=pltpu.SMEM)]
    specs += [pl.BlockSpec(memory_space=pltpu.VMEM)] * (len(args) - 1)
    many = isinstance(out, list)
    return pl.pallas_call(
        body,
        out_shape=out,
        in_specs=specs,
        out_specs=[pl.BlockSpec(memory_space=pltpu.VMEM)] * len(out) if many else pl.BlockSpec(memory_space=pltpu.VMEM),
        compiler_params=pltpu.CompilerParams(vmem_limit_bytes=20 * 2**20),
    )(*args)


def ring_z(x):
    part = x.shape[-2] // 5 * 3
    up = down = x
    ups, downs = [], []
    for _ in range(1, 4):
        up, down = send(up, ZUP), send(down, ZDOWN)
        ups.append(up)
        downs.append(down)
    last = send(up[..., :part, :], ZUP), send(down[..., part:, :], ZDOWN)
    return [x, *ups, *downs, *last]


OFFSETS = [0, 7, 6, 5, 1, 2, 3, 4, 4]


def spot(ids, n, at_z, rows):
    at_x = (ids[3] * 2 + ids[1] + [0, 3, 1, 2][n]) % 4
    return at_x % 2, pl.multiple_of((at_x // 2 * 8 + at_z) * rows, rows)


def lay_tied(ids, *refs):
    tied = refs[-1]
    part = refs[0].shape[1] // 5
    for piece, offset in zip(refs[:8], OFFSETS[:7] + OFFSETS[8:]):
        first = piece.shape[1] - part
        for n in range(4):
            xl, start = spot(ids, n, (ids[2] + offset) % 8, 2 * part)
            tied[pl.ds(pl.multiple_of(start + xl * part, part), part)] = piece[n, first:]


def lay_rest(ids, *refs):
    near, jump = refs[-2:]
    part = refs[0].shape[1] // 5
    rows = 2 * part
    for piece, offset, first in zip(refs[:9], OFFSETS, [0] * 8 + [3]):
        for n in range(4):
            xl, start = spot(ids, n, (ids[2] + offset) % 8, rows)
            for block in range(piece.shape[1] // part):
                number = first + block
                if number < 4:
                    begin = pl.multiple_of(start + number % 2 * part, part)
                    near[number // 2, xl, pl.ds(begin, part)] = piece[n, block * part : (block + 1) * part]
    for n, plane in enumerate(refs[9:13]):
        for at_z in range(8):
            xl, start = spot(ids, n, at_z, rows)
            jump[xl, pl.ds(start, rows)] = plane[at_z]


def wide(core, own, other, s, half):
    a, b = own[:, s * half : (s + 1) * half], other[:, s * half : (s + 1) * half]
    low = jnp.where(core == 0, a, b)
    high = jnp.where(core == 0, b, a)
    return jnp.concatenate([low, high], axis=1)


def forward_body(stage, ids, own, other, old, near, jump, tied, beyond, near_from, *outs):
    y, core = ids[0], ids[4]
    half = own.shape[1] // 2
    width = 2 * half
    top = wide(core, own[...], other[...], 0, half).astype(BF)
    here, there = dot(top, tied[...], NT), dot(top, beyond[...], NT)
    low, high = jnp.where(core == 0, here, there), jnp.where(core == 0, there, here)
    bottom = wide(core, own[...], other[...], 1, half) - jnp.concatenate([low, high], axis=1)
    new = jnp.concatenate([top, bottom.astype(BF)], axis=1)
    kept = jnp.where(y == stage, new, old[...])
    outs[0][...] = kept
    if stage == 3:
        return
    source = kept if stage < 2 else jnp.where(y == 3, near_from[...], kept)

    def section(t, carry):
        total = dot(source[:, :width], near[t, 0], NT) + dot(source[:, width:], near[t, 1], NT)
        outs[1][:, pl.ds(pl.multiple_of(t * half, half), half)] = total
        return carry

    lax.fori_loop(0, 2, section, 0)
    if stage == 0:
        outs[1][:, width:] = dot(kept[:, :width], jump[0], NT) + dot(kept[:, width:], jump[1], NT)


def near_body(ids, source, near, out):
    half = source.shape[1] // 2
    width = 2 * half
    a, b = source[:, :half], source[:, half:]

    def column(c, carry):
        at = pl.ds(pl.multiple_of(c * width, width), width)
        out[:, at] = dot(a, near[0, c], NN) + dot(b, near[1, c], NN)
        return carry

    lax.fori_loop(0, 2, column, 0)


def jump_body(ids, source, jump, out):
    width = jump.shape[2]

    def column(c, carry):
        out[:, pl.ds(pl.multiple_of(c * width, width), width)] = dot(source[...], jump[c], NN)
        return carry

    lax.fori_loop(0, 2, column, 0)


def solve_body(stage, ids, back, own, other, old, tied, beyond, jump, *outs):
    y, core = ids[0], ids[4]
    width = back.shape[1] // 2
    half = width // 2
    u = back[...] - (own[...].astype(F32) + other[...].astype(F32))
    x1 = u[:, width:]
    here = jnp.where(core == 0, x1[:, :half], x1[:, half:]).astype(BF)
    there = jnp.where(core == 0, x1[:, half:], x1[:, :half]).astype(BF)
    x0 = u[:, :width] - (dot(here, tied[...], NN) + dot(there, beyond[...], NN))
    kept = jnp.where(y == 3 - stage, jnp.concatenate([x0, x1], axis=1), old[...])
    outs[0][...] = kept
    if stage == 3:
        return
    parts = [
        jnp.where(core == 0, kept[:, s * width : s * width + half], kept[:, s * width + half : (s + 1) * width])
        for s in range(2)
    ]
    outs[1][...] = jnp.concatenate(parts, axis=1).astype(BF)
    if stage == 0:
        for c in range(2):
            outs[2][:, c * width : (c + 1) * width] = dot(parts[1].astype(BF), jump[c], NN)


def solve(rhs, coupling, diag_inverse):
    sec = lax.axis_index("sec")
    row = lax.axis_index("row")
    y, xl = sec // 2, sec % 2
    z, xh, core = row // 4, (row // 2) % 2, row % 2
    ids = jnp.stack([y, xl, z, xh, core]).astype(jnp.int32)
    rows, total = rhs.shape
    width = diag_inverse.shape[1]
    half = width // 2
    cols = total // ROW

    slot = jnp.arange(width)
    i, rest = slot % rows, slot // rows
    natural = ((rest % 8) * 4 + ((rest // 8) % 2) * 2 + rest // 16) * rows + i
    pick = (jnp.arange(width)[:, None] == natural[None, :]).astype(BF)
    m = dot(coupling.reshape(SEC * rows, width), diag_inverse[0], NN).astype(BF)
    m = dot(m, pick, NN).astype(BF).reshape(SEC, rows, width)
    inverse = dot(diag_inverse[0], pick, NN).astype(BF)

    def blocks(first, count):
        return lax.dynamic_slice_in_dim(m, first, count, 0)

    far = send(m[6:8], YB)
    inner = blocks(2 * y + 1, 1)[0]
    given = send(inner[rows // 2 :], XL)
    close = lax.ppermute(blocks(5 + 2 * (y % 2), 1), "sec", [(0, 2), (1, 3), (2, 6), (3, 7)])
    next_pair = jnp.where(y == 3, far, blocks(jnp.minimum(2 * y + 2, 6), 2))
    skip = jnp.where(y == 0, m[4], jnp.where(y == 2, far[0], close[0]))
    inner = jnp.where(xl == 0, inner[: rows // 2], given)

    lanes = rhs.T.reshape(8, 2, 2, cols, rows).transpose(2, 1, 0, 3, 4).reshape(ROW, cols * rows // 128, 128)
    mine = lax.all_to_all(lanes, BOTH, 0, 0, axis_index_groups=PLANES, tiled=True)
    mine = mine.reshape(2, 16, cols, rows)
    mine = mine.transpose(2, 0, 1, 3).reshape(cols, width)

    unit = jnp.concatenate([next_pair.reshape(2 * rows, width), inner], axis=0)
    unit = jnp.stack([unit, send(unit, XP), send(unit, XM), send(unit, XH)])
    plane = lax.all_to_all(jnp.broadcast_to(skip, (8, rows, width)), BOTH, 0, 0, axis_index_groups=RINGS, tiled=True)
    planes = [plane, send(plane, XP), send(plane, XM), send(plane, XH)]
    pieces = ring_z(unit) + planes
    pieces = [pltpu.with_memory_space_constraint(p, pltpu.VMEM) for p in pieces]
    away = send(inverse, [(a, b) for a, b in CROSS if a != b])
    inverse = jnp.where(core == xl, inverse, away)
    early = jnp.where(core == 0, jnp.ones((8, 128), F32), 0.0)
    tied = call(lay_tied, pltpu.VMEM((half, width), BF), ids, *pieces[:7], pieces[8], mine, inverse, early)
    beyond = pltpu.with_memory_space_constraint(send(tied, CORE), pltpu.VMEM)
    shapes = [pltpu.VMEM((2, 2, half, width), BF), pltpu.VMEM((2, half, width), BF)]
    near, jump = call(lay_rest, shapes, ids, *pieces)

    def struct(n, dtype):
        return jax.ShapeDtypeStruct((cols, n), dtype)

    zero_z = jnp.zeros((cols, 2 * width), BF)
    kept, got_z, resid, stash, ours = zero_z, zero_z, mine, None, None
    for stage in range(4):
        shapes = [struct(2 * width, BF)]
        shapes += [struct(width + half if stage == 0 else width, F32)] if stage < 3 else []
        across = send(resid, CORE)
        if 0 < stage < 3:
            leap = dot(got_z[:, :width], jump[0], NT) + dot(got_z[:, width:], jump[1], NT)
        got = call(functools.partial(forward_body, stage), shapes, ids, resid, across, kept, near, jump, tied, beyond, got_z)
        kept = got[0]
        if stage == 3:
            break
        update = got[1][:, :width]
        if stage == 0:
            leap = got[1][:, width:]
        if stage == 0:
            sent = jnp.concatenate([update.astype(BF), leap.astype(BF), kept], axis=1)
        elif stage == 1:
            update = update + jnp.concatenate([stash.astype(F32), leap], axis=1)
            sent = jnp.concatenate([update.astype(BF), kept], axis=1)
        else:
            ours = update
            update = update + jnp.concatenate([leap, jnp.zeros_like(leap)], axis=1)
            sent = jnp.concatenate([update.astype(BF), got_z], axis=1)
        arrived = send(sent, SWAPS[stage])
        acc, got_z = arrived[:, :width].astype(F32), arrived[:, -2 * width :]
        if stage == 0:
            stash = arrived[:, width : width + half]
        if stage == 2:
            late = dot(got_z[:, :width], jump[0], NT) + dot(got_z[:, width:], jump[1], NT)
            acc = acc + ours + jnp.concatenate([jnp.zeros_like(late), late], axis=1)
        resid = mine - acc

    def mine_of(pair):
        return jnp.where(core == 0, pair[:, :width], pair[:, width:])

    solved = dot(mine_of(kept), inverse, NT)
    back = dot(solved.astype(BF), inverse, NN)
    other = send(back, CORE)
    back = jnp.concatenate([jnp.where(core == 0, back, other), jnp.where(core == 0, other, back)], axis=1)

    zero = jnp.zeros((cols, 2 * width), F32)
    answer, halves, own, other = zero, None, zero.astype(BF), zero.astype(BF)
    arrived, ours = None, None
    for stage in range(4):
        if stage > 0:
            got_x = arrived[:, :width]
            got_c = arrived[:, width : 3 * width].astype(F32)
            if stage == 1:
                sources = jnp.where(y == 3, halves, got_x), got_x[:, :half]
            elif stage == 2:
                sources = got_x, got_x[:, half:]
            else:
                sources = got_x, arrived[:, 3 * width :]
            by_near = call(near_body, struct(2 * width, F32), ids, sources[0], near)
            by_jump = call(jump_body, struct(2 * width, F32), ids, sources[1], jump)
            if stage == 1:
                own = by_near
                give = jnp.where(y == 3, by_near, by_jump + got_c)
            elif stage == 2:
                own, ours, give = by_near + got_c, got_c, by_jump
            else:
                own = by_near + by_jump + got_c + ours
            own = own.astype(BF)
            other = send(own, CORE)
        shapes = [struct(2 * width, F32)]
        shapes += [struct(width, BF)] if stage < 3 else []
        shapes += [struct(2 * width, F32)] if stage == 0 else []
        got = call(functools.partial(solve_body, stage), shapes, ids, back, own, other, answer, tied, beyond, jump)
        answer = got[0]
        if stage == 3:
            break
        halves = got[1]
        if stage == 0:
            give = got[2]
        sent = [halves, give.astype(BF)] + ([got_x[:, :half]] if stage == 2 else [])
        arrived = send(jnp.concatenate(sent, axis=1), SWAPS[stage])

    final = send(jnp.concatenate([mine_of(answer), solved], axis=1).astype(BF), CROSS)
    solved = final[:, width:].reshape(cols, ROW, rows).transpose(1, 0, 2)
    final = final[:, :width].reshape(cols, 2, 2, 8, rows).transpose(3, 2, 1, 0, 4).reshape(ROW, cols, rows)
    final = jnp.concatenate([final, solved], axis=1).reshape(ROW, 2 * cols * rows // 128, 128)
    got = lax.all_to_all(final, "row", 0, 0, tiled=True).astype(F32)
    got = got.reshape(ROW, 2, cols, rows).transpose(1, 3, 0, 2).reshape(2, rows, total)
    return (got[0], got[1])


def solution(mesh):
    return jax.shard_map(
        solve,
        mesh=mesh,
        in_specs=(P(("sec", "row"), None), P(None, "row", "sec"), P("sec", None, None)),
        out_specs=(P(("sec", "row"), None), P(("sec", "row"), None)),
        check_vma=False,
    )
```

```python
import functools

import jax
import jax.numpy as jnp
from jax import lax
from jax.experimental import pallas as pl
from jax.experimental.pallas import tpu as pltpu
from jax.sharding import PartitionSpec as P


BF = jnp.bfloat16
F32 = jnp.float32
SEC, ROW = 8, 32
NT = (((1,), (1,)), ((), ()))
NN = (((1,), (0,)), ((), ()))
BOTH = ("sec", "row")


def place(dev):
    sec, row = divmod(dev, ROW)
    return sec // 2, sec % 2, row // 4, (row // 2) % 2, row % 2


def device(y, xl, z, xh, core):
    return (y * 2 + xl) * ROW + z * 4 + xh * 2 + core


def moved(move):
    return [(d, device(*move(*place(d)))) for d in range(SEC * ROW)]


XL = moved(lambda y, xl, z, xh, k: (y, 1 - xl, z, xh, k))
XH = moved(lambda y, xl, z, xh, k: (y, xl, z, 1 - xh, k))
CORE = moved(lambda y, xl, z, xh, k: (y, xl, z, xh, 1 - k))
ZUP = moved(lambda y, xl, z, xh, k: (y, xl, (z + 1) % 8, xh, k))
ZDOWN = moved(lambda y, xl, z, xh, k: (y, xl, (z - 1) % 8, xh, k))
XP = moved(lambda y, xl, z, xh, k: (y, 1 - xl, z, (xh + xl) % 2, k))
XM = moved(lambda y, xl, z, xh, k: (y, 1 - xl, z, (xh + 1 - xl) % 2, k))
CROSS = moved(lambda y, xl, z, xh, k: (y, k, z, xh, xl))
YA = moved(lambda y, xl, z, xh, k: (y ^ 1, xl, z, xh, k))
YB = moved(lambda y, xl, z, xh, k: ({0: 3, 1: 2, 2: 1, 3: 0}[y], xl, z, xh, k))
PLANES = [
    [device(y, xl, z, xh, k) for xl in range(2) for xh in range(2) for z in range(8)]
    for y in range(4)
    for k in range(2)
]
RINGS = [
    [device(y, xl, z, xh, k) for z in range(8)] for y in range(4) for xl in range(2) for xh in range(2) for k in range(2)
]
SWAPS = [YA, YB, YA]


def send(x, pairs):
    return lax.ppermute(x, BOTH, pairs)


def dot(a, b, dims):
    return lax.dot_general(a, b, dims, preferred_element_type=F32)


def call(body, out, *args):
    specs = [pl.BlockSpec(memory_space=pltpu.SMEM)]
    specs += [pl.BlockSpec(memory_space=pltpu.VMEM)] * (len(args) - 1)
    many = isinstance(out, list)
    return pl.pallas_call(
        body,
        out_shape=out,
        in_specs=specs,
        out_specs=[pl.BlockSpec(memory_space=pltpu.VMEM)] * len(out) if many else pl.BlockSpec(memory_space=pltpu.VMEM),
        compiler_params=pltpu.CompilerParams(vmem_limit_bytes=20 * 2**20),
    )(*args)


def ring_z(x):
    part = x.shape[-2] // 5 * 3
    up = down = x
    ups, downs = [], []
    for _ in range(1, 4):
        up, down = send(up, ZUP), send(down, ZDOWN)
        ups.append(up)
        downs.append(down)
    last = send(up[..., :part, :], ZUP), send(down[..., part:, :], ZDOWN)
    return [x, *ups, *downs, *last]


def lay_all(ids, *refs):
    near, jump, tied = refs[-3:]
    z, x = ids[2], ids[3] * 2 + ids[1]
    part = refs[0].shape[1] // 5
    rows = 2 * part

    def spot(n, at_z):
        at_x = (x + [0, 3, 1, 2][n]) % 4
        return at_x % 2, pl.multiple_of((at_x // 2 * 8 + at_z) * rows, rows)

    for piece, offset, first in zip(refs[:9], [0, 7, 6, 5, 1, 2, 3, 4, 4], [0] * 8 + [3]):
        for n in range(4):
            xl, start = spot(n, (z + offset) % 8)
            for block in range(piece.shape[1] // part):
                number = first + block
                rows_in = slice(block * part, (block + 1) * part)
                if number < 4:
                    begin = pl.multiple_of(start + number % 2 * part, part)
                    near[number // 2, xl, pl.ds(begin, part)] = piece[n, rows_in]
                else:
                    tied[pl.ds(pl.multiple_of(start + xl * part, part), part)] = piece[n, rows_in]
    for n, plane in enumerate(refs[9:13]):
        for at_z in range(8):
            xl, start = spot(n, at_z)
            jump[xl, pl.ds(start, rows)] = plane[at_z]


def lay_tied(ids, own, other, out):
    half = own.shape[0]
    out[pl.ds(pl.multiple_of(ids[4] * half, half), half)] = own[...]
    out[pl.ds(pl.multiple_of((1 - ids[4]) * half, half), half)] = other[...]


def wide(core, own, other, s, half):
    a, b = own[:, s * half : (s + 1) * half], other[:, s * half : (s + 1) * half]
    low = jnp.where(core == 0, a, b)
    high = jnp.where(core == 0, b, a)
    return jnp.concatenate([low, high], axis=1)


def forward_body(stage, ids, own, other, old, near, jump, tied, near_from, *outs):
    y, core = ids[0], ids[4]
    half = own.shape[1] // 2
    width = 2 * half
    top = wide(core, own[...], other[...], 0, half).astype(BF)
    bottom = wide(core, own[...], other[...], 1, half) - dot(top, tied[...], NT)
    new = jnp.concatenate([top, bottom.astype(BF)], axis=1)
    kept = jnp.where(y == stage, new, old[...])
    outs[0][...] = kept
    if stage == 3:
        return
    source = kept if stage < 2 else jnp.where(y == 3, near_from[...], kept)

    def section(t, carry):
        total = dot(source[:, :width], near[t, 0], NT) + dot(source[:, width:], near[t, 1], NT)
        outs[1][:, pl.ds(pl.multiple_of(t * half, half), half)] = total
        return carry

    lax.fori_loop(0, 2, section, 0)
    if stage == 0:
        outs[1][:, width:] = dot(kept[:, :width], jump[0], NT) + dot(kept[:, width:], jump[1], NT)


def near_body(ids, source, near, out):
    half = source.shape[1] // 2
    width = 2 * half
    a, b = source[:, :half], source[:, half:]

    def column(c, carry):
        at = pl.ds(pl.multiple_of(c * width, width), width)
        out[:, at] = dot(a, near[0, c], NN) + dot(b, near[1, c], NN)
        return carry

    lax.fori_loop(0, 2, column, 0)


def jump_body(ids, source, jump, out):
    width = jump.shape[2]

    def column(c, carry):
        out[:, pl.ds(pl.multiple_of(c * width, width), width)] = dot(source[...], jump[c], NN)
        return carry

    lax.fori_loop(0, 2, column, 0)


def solve_body(stage, ids, back, own, other, old, tied, jump, *outs):
    y, core = ids[0], ids[4]
    width = back.shape[1] // 2
    half = width // 2
    u = back[...] - (own[...].astype(F32) + other[...].astype(F32))
    x1 = u[:, width:]
    x0 = u[:, :width] - dot(x1.astype(BF), tied[...], NN)
    kept = jnp.where(y == 3 - stage, jnp.concatenate([x0, x1], axis=1), old[...])
    outs[0][...] = kept
    if stage == 3:
        return
    parts = [
        jnp.where(core == 0, kept[:, s * width : s * width + half], kept[:, s * width + half : (s + 1) * width])
        for s in range(2)
    ]
    outs[1][...] = jnp.concatenate(parts, axis=1).astype(BF)
    if stage == 0:
        jump_body(ids, parts[1].astype(BF), jump, outs[2])


def solve(rhs, coupling, diag_inverse):
    sec = lax.axis_index("sec")
    row = lax.axis_index("row")
    y, xl = sec // 2, sec % 2
    z, xh, core = row // 4, (row // 2) % 2, row % 2
    ids = jnp.stack([y, xl, z, xh, core]).astype(jnp.int32)
    rows, total = rhs.shape
    width = diag_inverse.shape[1]
    half = width // 2
    cols = total // ROW

    slot = jnp.arange(width)
    i, rest = slot % rows, slot // rows
    natural = ((rest % 8) * 4 + ((rest // 8) % 2) * 2 + rest // 16) * rows + i
    pick = (jnp.arange(width)[:, None] == natural[None, :]).astype(BF)
    m = dot(coupling.reshape(SEC * rows, width), diag_inverse[0], NN).astype(BF)
    m = dot(m, pick, NN).astype(BF).reshape(SEC, rows, width)
    inverse = dot(diag_inverse[0], pick, NN).astype(BF)

    def blocks(first, count):
        return lax.dynamic_slice_in_dim(m, first, count, 0)

    far = send(m[6:8], YB)
    inner = blocks(2 * y + 1, 1)[0]
    given = send(inner[rows // 2 :], XL)
    close = lax.ppermute(blocks(5 + 2 * (y % 2), 1), "sec", [(0, 2), (1, 3), (2, 6), (3, 7)])
    next_pair = jnp.where(y == 3, far, blocks(jnp.minimum(2 * y + 2, 6), 2))
    skip = jnp.where(y == 0, m[4], jnp.where(y == 2, far[0], close[0]))
    inner = jnp.where(xl == 0, inner[: rows // 2], given)

    lanes = rhs.T.reshape(8, 2, 2, cols, rows).transpose(2, 1, 0, 3, 4).reshape(ROW, cols * rows // 128, 128)
    mine = lax.all_to_all(lanes, BOTH, 0, 0, axis_index_groups=PLANES, tiled=True)
    mine = mine.reshape(2, 16, cols, rows).transpose(2, 0, 1, 3).reshape(cols, width)

    unit = jnp.concatenate([next_pair.reshape(2 * rows, width), inner], axis=0)
    unit = jnp.stack([unit, send(unit, XP), send(unit, XM), send(unit, XH)])
    plane = lax.all_to_all(jnp.broadcast_to(skip, (8, rows, width)), BOTH, 0, 0, axis_index_groups=RINGS, tiled=True)
    planes = [plane, send(plane, XP), send(plane, XM), send(plane, XH)]
    pieces = ring_z(unit) + planes
    pieces = [pltpu.with_memory_space_constraint(p, pltpu.VMEM) for p in pieces]
    shapes = [pltpu.VMEM((2, 2, half, width), BF), pltpu.VMEM((2, half, width), BF), pltpu.VMEM((half, width), BF)]
    away = send(inverse, [(a, b) for a, b in CROSS if a != b])
    inverse = jnp.where(core == xl, inverse, away)
    early = jnp.where(core == 0, jnp.ones((8, 128), F32), 0.0)
    near, jump, tied = call(lay_all, shapes, ids, *pieces, mine, inverse, early)
    tied = call(lay_tied, pltpu.VMEM((width, width), BF), ids, tied, send(tied, CORE))

    def struct(n, dtype):
        return jax.ShapeDtypeStruct((cols, n), dtype)

    zero_z = jnp.zeros((cols, 2 * width), BF)
    kept, got_z, resid, stash, ours = zero_z, zero_z, mine, None, None
    for stage in range(4):
        shapes = [struct(2 * width, BF)]
        shapes += [struct(width + half if stage == 0 else width, F32)] if stage < 3 else []
        across = send(resid, CORE)
        if 0 < stage < 3:
            leap = dot(got_z[:, :width], jump[0], NT) + dot(got_z[:, width:], jump[1], NT)
        got = call(functools.partial(forward_body, stage), shapes, ids, resid, across, kept, near, jump, tied, got_z)
        kept = got[0]
        if stage == 3:
            break
        update = got[1][:, :width]
        if stage == 0:
            leap = got[1][:, width:]
        if stage == 0:
            sent = jnp.concatenate([update.astype(BF), leap.astype(BF), kept], axis=1)
        elif stage == 1:
            update = update + jnp.concatenate([stash.astype(F32), leap], axis=1)
            sent = jnp.concatenate([update.astype(BF), kept], axis=1)
        else:
            ours = update
            update = update + jnp.concatenate([leap, jnp.zeros_like(leap)], axis=1)
            sent = jnp.concatenate([update.astype(BF), got_z], axis=1)
        arrived = send(sent, SWAPS[stage])
        acc, got_z = arrived[:, :width].astype(F32), arrived[:, -2 * width :]
        if stage == 0:
            stash = arrived[:, width : width + half]
        if stage == 2:
            late = dot(got_z[:, :width], jump[0], NT) + dot(got_z[:, width:], jump[1], NT)
            acc = acc + ours + jnp.concatenate([jnp.zeros_like(late), late], axis=1)
        resid = mine - acc

    def mine_of(pair):
        return jnp.where(core == 0, pair[:, :width], pair[:, width:])

    solved = dot(mine_of(kept), inverse, NT)
    back = dot(solved.astype(BF), inverse, NN)
    solved = send(solved.astype(BF), CROSS)
    other = send(back, CORE)
    back = jnp.concatenate([jnp.where(core == 0, back, other), jnp.where(core == 0, other, back)], axis=1)

    zero = jnp.zeros((cols, 2 * width), F32)
    answer, halves, own, other = zero, None, zero.astype(BF), zero.astype(BF)
    arrived, ours = None, None
    for stage in range(4):
        if stage > 0:
            got_x = arrived[:, :width]
            got_c = arrived[:, width : 3 * width].astype(F32)
            if stage == 1:
                sources = jnp.where(y == 3, halves, got_x), got_x[:, :half]
            elif stage == 2:
                sources = got_x, got_x[:, half:]
            else:
                sources = got_x, arrived[:, 3 * width :]
            by_near = call(near_body, struct(2 * width, F32), ids, sources[0], near)
            by_jump = call(jump_body, struct(2 * width, F32), ids, sources[1], jump)
            if stage == 1:
                own = by_near
                give = jnp.where(y == 3, by_near, by_jump + got_c)
            elif stage == 2:
                own, ours, give = by_near + got_c, got_c, by_jump
            else:
                own = by_near + by_jump + got_c + ours
            own = own.astype(BF)
            other = send(own, CORE)
        shapes = [struct(2 * width, F32)]
        shapes += [struct(width, BF)] if stage < 3 else []
        shapes += [struct(2 * width, F32)] if stage == 0 else []
        got = call(functools.partial(solve_body, stage), shapes, ids, back, own, other, answer, tied, jump)
        answer = got[0]
        if stage == 3:
            break
        halves = got[1]
        if stage == 0:
            give = got[2]
        sent = [halves, give.astype(BF)] + ([got_x[:, :half]] if stage == 2 else [])
        arrived = send(jnp.concatenate(sent, axis=1), SWAPS[stage])

    low, high = answer[:, :width].astype(BF), answer[:, width:].astype(BF)
    there = send(jnp.where(xl == 0, high, low), XL)
    final = jnp.where(core == xl, jnp.where(xl == 0, low, high), there)
    solved = solved.reshape(cols, ROW, rows).transpose(1, 0, 2)
    final = final.reshape(cols, 2, 2, 8, rows).transpose(3, 2, 1, 0, 4).reshape(ROW, cols, rows)
    final = jnp.concatenate([final, solved], axis=1).reshape(ROW, 2 * cols * rows // 128, 128)
    got = lax.all_to_all(final, "row", 0, 0, tiled=True).astype(F32)
    got = got.reshape(ROW, 2, cols, rows).transpose(1, 3, 0, 2).reshape(2, rows, total)
    return (got[0], got[1])


def solution(mesh):
    return jax.shard_map(
        solve,
        mesh=mesh,
        in_specs=(P(("sec", "row"), None), P(None, "row", "sec"), P("sec", None, None)),
        out_specs=(P(("sec", "row"), None), P(("sec", "row"), None)),
        check_vma=False,
    )
```
